32 devices in a mesh: row: 2 (over core), sector: 4 (over z), slab: 4 (over y, x).
Axes of the slice: x: 2, y: 2, z: 4, core: 2. Of those that a mesh axis runs over, the one named last changes fastest.
Arguments:
- state: float32 [2, 5, 32, 128, 128], P('row', None, 'slab', 'sector'), may hold values from -6 to 6
- source: float32 [2, 5, 32, 128, 128], P('row', None, 'slab', 'sector'), may hold values from -6 to 6
- diag_inverse: float32 [2, 5, 5, 32, 128, 128], P('row', None, None, 'slab', 'sector'), may hold values from -1 to 1
- jac_axial: float32 [2, 5, 5], P('row'), may hold values from -1 to 2
- jac_cross: float32 [2, 2, 5, 5], P('row'), may hold values from -2.5 to 2.5
- owner: int32 [128], replicated, may hold values from 0 to 127, as said below
Outputs:
- residual: float32 [2, 5, 32, 128, 128], P('row', None, 'slab', 'sector')
- new_state: float32 [2, 5, 32, 128, 128], P('row', None, 'slab', 'sector')
The draws below stay inside these ranges and needn't reach their ends.
Inputs may be any that keep to these rules, and one draw needn't show every extreme that they name: owner is a permutation; for some whole s, the columns b * 32 to b * 32 + 31 of the rotor face exactly the stator columns s + b * 32 to s + b * 32 + 31, taken modulo 128, for every b.
All inputs are finite; a program needn't handle non-finite values.
Results may differ from the reference program's by a relative error of at most 0.0001.
Values sent between devices are 32-bit elements; how exact they have to be, the bound alone decides.
A program may use at most 64 MiB of HBM per device.

```python
import jax
import jax.numpy as jnp
from jax import lax

VARS = 5
C = 32
R = 128
AXIAL_PLANES = 32
NC = 128


def draw_diag_inverse(key, part):
    first, second, third, fourth = jax.random.split(jax.random.fold_in(key, 11), 4)
    doubling_level = jax.random.uniform(first, (2, AXIAL_PLANES, NC, R), jnp.float32, 0.92, 1.0)
    plane_positions = jax.random.randint(second, (2, 3), 0, AXIAL_PLANES)
    sweep_group = jnp.any(jnp.arange(AXIAL_PLANES)[None, :, None] == plane_positions[:, None, :], axis=2)
    doubling_level = doubling_level * jnp.where(sweep_group, 0.6, 1.0)[:, :, None, None]
    vary = jax.random.uniform(fourth, (2, 5, AXIAL_PLANES, NC, R), jnp.float32, 0.85, 1.0)
    diagonal = doubling_level[:, None] * vary
    noise = 0.06 * jax.random.normal(third, (2, 5, 5, AXIAL_PLANES, NC, R), jnp.float32)
    identity = jnp.eye(5, dtype=jnp.float32)[None, :, :, None, None, None]
    return identity * diagonal[:, :, None] + (1.0 - identity) * noise


def draw_jac_axial(key, part):
    first, second = jax.random.split(jax.random.fold_in(key, 17), 2)
    rates = jax.random.uniform(first, (2, 5), jnp.float32, 0.9, 0.98)
    noise = 0.08 * jax.random.normal(second, (2, 5, 5), jnp.float32)
    identity = jnp.eye(5, dtype=jnp.float32)[None]
    return identity * (2.0 * rates)[:, :, None] + (1.0 - identity) * noise


def draw_owner(key, part):
    first, second = jax.random.split(jax.random.fold_in(key, 23), 2)
    offset = jax.random.randint(first, (), 0, NC)
    blocks = NC // C
    scores = jax.random.randint(second, (blocks, C), 0, 2 ** 20) * C + jnp.arange(C, dtype=jnp.int32)[None, :]
    within = jnp.argsort(scores, axis=1).astype(jnp.int32)
    starts = jnp.arange(blocks, dtype=jnp.int32)[:, None] * C
    return ((offset + starts + within) % NC).reshape(NC).astype(jnp.int32)


def steps_of(own_key, dims, cuts, smallest, high):
    def one(dim, blocks):
        draws = jax.random.uniform(jax.random.fold_in(jax.random.fold_in(own_key, 6), dim), (blocks,), jnp.float32, smallest / len(cuts), high / len(cuts))
        return jnp.repeat(jnp.exp(draws), dims[dim] // blocks).reshape((-1,) + (1,) * (len(dims) - dim - 1))

    loudness = one(*cuts[0])
    for cut in cuts[1:]:
        loudness = loudness * one(*cut)
    return loudness


def normal_values(stream_key, dims, scale, limit, pieces=(), kind=jnp.bfloat16):
    factor_of = steps_of(stream_key, dims, pieces, -0.22, 0.18) if pieces else 1.0
    entries = jax.random.normal(stream_key, dims, jnp.float32) * scale * factor_of
    return jnp.minimum(jnp.maximum(entries, -limit), limit).astype(kind)


def setup_inputs(seed: int = 0) -> dict:
    seeds = jax.random.split(jax.random.key(seed), 7)
    return {
        "state": normal_values(seeds[0], (2, VARS, AXIAL_PLANES, NC, R), 1.0, 6.0, ((0, 2), (2, 4), (3, 4)), jnp.float32),
        "source": normal_values(seeds[1], (2, VARS, AXIAL_PLANES, NC, R), 1.0, 6.0, ((0, 2), (2, 4), (3, 4)), jnp.float32),
        "diag_inverse": draw_diag_inverse(jax.random.fold_in(seeds[6], 71), 0),
        "jac_axial": draw_jac_axial(jax.random.fold_in(seeds[6], 71), 0),
        "jac_cross": normal_values(seeds[4], (2, 2, VARS, VARS), VARS ** -0.5, 2.5, ((0, 2),), jnp.float32),
        "owner": draw_owner(jax.random.fold_in(seeds[6], 71), 0),
    }


exact_mode = lax.Precision.HIGHEST


def mix_const(matrix, field):
    return jnp.einsum('ij,j...->i...', matrix, field, precision=exact_mode)


def per_cell(blocks, field):
    return jnp.sum(blocks * field[None], axis=1)


def forward_sweep(residual, inverse, axial, entering):
    planes = residual.shape[1]

    def advance(plane_at, carried):
        previous, output = carried
        block = lax.dynamic_index_in_dim(inverse, plane_at, 2, keepdims=False)
        value = lax.dynamic_index_in_dim(residual, plane_at, 1, keepdims=False)
        present_plane = per_cell(block, value + 0.5 * mix_const(axial, previous))
        output = lax.dynamic_update_index_in_dim(output, present_plane, plane_at, 1)
        return present_plane, output

    final_plane, output = lax.fori_loop(0, planes, advance, (entering, jnp.zeros_like(residual)))
    return output


def backward_sweep(provisional, inverse, axial, entering):
    planes = provisional.shape[1]

    def advance(step_at, carried):
        following, output = carried
        plane_at = planes - 1 - step_at
        block = lax.dynamic_index_in_dim(inverse, plane_at, 2, keepdims=False)
        value = lax.dynamic_index_in_dim(provisional, plane_at, 1, keepdims=False)
        present_plane = value - per_cell(block, 0.5 * mix_const(axial, following))
        output = lax.dynamic_update_index_in_dim(output, present_plane, plane_at, 1)
        return present_plane, output

    final_plane, output = lax.fori_loop(0, planes, advance, (entering, jnp.zeros_like(provisional)))
    return output


def flux_residual(field, source, axial, circular, radial_jac, below, above):
    axial_padded = jnp.concatenate([below[:, None], field, above[:, None]], axis=1)
    axial_diff = axial_padded[:, 2:] - axial_padded[:, :-2]
    cycle_diff = jnp.roll(field, -1, axis=2) - jnp.roll(field, 1, axis=2)
    radial = jnp.pad(field, ((0, 0), (0, 0), (0, 0), (1, 1)))
    radial_diff = radial[..., 2:] - radial[..., :-2]
    return source - 0.5 * (mix_const(axial, axial_diff) + mix_const(circular, cycle_diff) + mix_const(radial_jac, radial_diff))


def reference(state, source, diag_inverse, jac_axial, jac_cross, owner):
    zeros_plane = jnp.zeros_like(state[0][:, 0])
    rotor_above = jnp.take(state[1][:, 0], owner, axis=1)
    stator_below = zeros_plane.at[:, owner].set(state[0][:, -1])
    bounds = ((zeros_plane, rotor_above), (stator_below, zeros_plane))
    residuals = []
    updated = []
    for blade_row in range(2):
        field = state[blade_row]
        residual = flux_residual(field, source[blade_row], jac_axial[blade_row], jac_cross[blade_row, 0], jac_cross[blade_row, 1], bounds[blade_row][0], bounds[blade_row][1])
        provisional = forward_sweep(residual, diag_inverse[blade_row], jac_axial[blade_row], zeros_plane)
        update = backward_sweep(provisional, diag_inverse[blade_row], jac_axial[blade_row], zeros_plane)
        residuals.append(residual)
        updated.append(field + update)
    return jnp.stack(residuals), jnp.stack(updated)
```

```python
import functools

import jax
import jax.numpy as jnp
from jax import lax
from jax.experimental import pallas as pl
from jax.experimental.pallas import tpu as pltpu
from jax.sharding import PartitionSpec as P

MESH = pl.DeviceIdType.MESH
PAD = 8
GROUP = 8


def total(terms):
    while len(terms) > 1:
        pairs = [a + b for a, b in zip(terms[::2], terms[1::2])]
        if len(terms) % 2:
            pairs.append(terms[-1])
        terms = pairs
    return terms[0]


def both(*conditions):
    return functools.reduce(jnp.logical_and, conditions)


def kernel(
    sectors, slabs,
    state, source, inverse, axial_in, cross_in, owner_in,
    res_out, state_out,
    axial, cross, owner, picks_wide, picks,
    q, src, inv, eff, prov, below, above, facing, entering, following, leaving, upd,
    local_sem, ax_send, ax_recv, se_send, se_recv,
    if_send, if_recv, fw_send, fw_recv, bw_send, bw_recv, sectors_in,
):
    nv, planes, columns, cells = src.shape
    groups = columns // GROUP
    row = lax.axis_index("row")
    sector = lax.axis_index("sector")
    slab = lax.axis_index("slab")
    rotor, stator = row == 0, row == 1
    has_low = slab > 0
    has_high = slab < slabs - 1
    is_first, is_last = slab == 0, slab == slabs - 1
    middle = both(has_low, has_high)
    outer = jnp.logical_or(is_first, is_last)
    rotor_top = both(rotor, is_last)
    stator_foot = both(stator, is_first)
    on_plane = jnp.logical_or(rotor_top, stator_foot)
    after = lax.rem(sector + 1, sectors)
    before = lax.rem(sector + sectors - 1, sectors)
    facing_slab = jnp.where(row == 0, 0, slabs - 1)
    body = pl.ds(PAD, columns)

    load_state = pltpu.make_async_copy(state.at[0], q.at[:, :, body], local_sem.at[0])
    load_state.start()
    load_axial = pltpu.make_async_copy(axial_in, axial, local_sem.at[4])
    load_axial.start()
    load_inverse = pltpu.make_async_copy(inverse.at[0], inv, local_sem.at[2])
    load_inverse.start()
    load_cross = pltpu.make_async_copy(cross_in, cross, local_sem.at[5])
    load_cross.start()
    load_owner = pltpu.make_async_copy(owner_in, owner, local_sem.at[3])
    load_owner.start()
    load_source = pltpu.make_async_copy(source.at[0], src, local_sem.at[1])
    load_source.start()

    barrier = pltpu.get_barrier_semaphore()

    def greet(**where):
        pl.semaphore_signal(barrier, inc=1, device_id=where, device_id_type=MESH)

    @pl.when(on_plane)
    def _():
        for other in range(sectors):
            greet(row=1 - row, sector=other, slab=facing_slab)

    @pl.when(has_high)
    def _():
        greet(slab=slab + 1)

    @pl.when(jnp.logical_or(stator, outer))
    def _():
        greet(sector=after)
        greet(sector=before)

    @pl.when(both(rotor, middle))
    def _():
        greet(row=1, sector=after)
        greet(row=1, sector=before)
        greet(row=1)

    peers = (
        has_low.astype(jnp.int32)
        + jnp.where(jnp.logical_or(stator, outer), 2, 0)
        + jnp.where(both(stator, middle), 3, 0)
        + jnp.where(on_plane, sectors, 0)
    )

    zero_plane = jnp.zeros((nv, columns, cells), jnp.float32)

    @pl.when(is_first)
    def _():
        entering[...] = zero_plane
        below[...] = zero_plane

    @pl.when(is_last)
    def _():
        following[...] = zero_plane
        above[...] = zero_plane

    move_picks = pltpu.make_async_copy(picks_wide, picks, local_sem.at[6])
    load_owner.wait()

    @pl.when(on_plane)
    def _():
        shape = (columns, owner.shape[1])
        ids = sector * columns + lax.broadcasted_iota(jnp.int32, shape, 0)
        everyone = lax.broadcasted_iota(jnp.int32, shape, 1)
        owners = jnp.broadcast_to(owner[...], shape)
        is_rotor = jnp.broadcast_to(row, shape) == 0
        hits = jnp.where(is_rotor, everyone, owners) == ids
        found = jnp.sum(
            jnp.where(hits, jnp.where(is_rotor, owners, everyone), 0), axis=1, keepdims=True
        )
        found = jnp.minimum(found, owner.shape[1] - 1)
        picks_wide[...] = jnp.broadcast_to(found, picks_wide.shape)
        move_picks.start()

    def remote(source_ref, target_ref, send, recv, **where):
        return pltpu.make_async_remote_copy(
            src_ref=source_ref, dst_ref=target_ref, send_sem=send, recv_sem=recv,
            device_id=where, device_id_type=MESH,
        )

    def facing_copy(plane_at, other):
        return remote(
            q.at[:, plane_at, body], facing.at[sector], if_send.at[other], if_recv.at[sector],
            row=1 - row, sector=other, slab=facing_slab,
        )

    def facing_arrival(other):
        return remote(
            q.at[:, 0, body], facing.at[other], if_send.at[other], if_recv.at[other],
            row=1 - row, sector=other, slab=facing_slab,
        )

    to_after = remote(
        q.at[:, :, pl.ds(PAD + columns - 1, 1)], q.at[:, :, pl.ds(PAD - 1, 1)],
        se_send.at[0], se_recv.at[0], sector=after,
    )
    to_before = remote(
        q.at[:, :, pl.ds(PAD, 1)], q.at[:, :, pl.ds(PAD + columns, 1)],
        se_send.at[1], se_recv.at[1], sector=before,
    )
    to_high = remote(
        q.at[:, planes - 1, body], below, ax_send.at[0], ax_recv.at[0], slab=slab + 1
    )
    to_low = remote(
        q.at[:, 0, body], above, ax_send.at[1], ax_recv.at[1], slab=slab - 1
    )

    def open_up():
        pl.semaphore_wait(barrier, peers)
        load_state.wait()

        @pl.when(has_low)
        def _():
            to_low.start()

        @pl.when(rotor_top)
        def _():
            for other in range(sectors):
                facing_copy(planes - 1, other).start()

        @pl.when(stator_foot)
        def _():
            for other in range(sectors):
                facing_copy(0, other).start()

        @pl.when(both(stator, middle))
        def _():
            pl.semaphore_signal(
                sectors_in, inc=1, device_id=dict(row=0), device_id_type=MESH
            )

    def products():
        load_axial.wait()
        load_inverse.wait()

        def effective(x, carry):
            for i in range(nv):
                blocks = [inv[i, j, x] for j in range(nv)]
                for k in range(nv):
                    eff[i, k, x] = total([blocks[j] * (0.5 * axial[j, 0, k]) for j in range(nv)])
            return carry

        lax.fori_loop(0, planes, effective, 0)

    far = sector >= sectors // 2
    early = both(rotor, jnp.logical_or(middle, both(is_last, far)))
    opens_at = jnp.where(early, 0, 2)

    def prepare(step, carry):
        pl.when(step == opens_at)(open_up)
        pl.when(step == 1)(products)
        return carry

    lax.fori_loop(0, 3, prepare, 0)

    @pl.when(both(rotor, middle))
    def _():
        pl.semaphore_wait(sectors_in, 1)

    to_after.start()
    to_before.start()
    load_cross.wait()
    load_source.wait()

    def columns_of(g):
        return pl.ds(pl.multiple_of(g * GROUP, GROUP), GROUP)

    def padded(g, shift=0):
        if shift:
            return pl.ds(PAD + g * GROUP + shift, GROUP)
        return pl.ds(pl.multiple_of(PAD + g * GROUP, GROUP), GROUP)

    lane = lax.broadcasted_iota(jnp.int32, (GROUP, cells), 1)
    no_cells = jnp.zeros((GROUP, cells), jnp.float32)

    def flux(g):
        at = columns_of(g)

        def one(x, carry):
            higher = jnp.minimum(x + 1, planes - 1)
            lower = jnp.maximum(x - 1, 0)
            sums = [None] * nv
            for v in range(nv):
                here = q[v, x, padded(g)]
                spans = (
                    jnp.where(x == planes - 1, no_cells, q[v, higher, padded(g)])
                    - jnp.where(x == 0, no_cells, q[v, lower, padded(g)]),
                    q[v, x, padded(g, 1)] - q[v, x, padded(g, -1)],
                    jnp.where(lane == cells - 1, 0.0, pltpu.roll(here, cells - 1, 1))
                    - jnp.where(lane == 0, 0.0, pltpu.roll(here, 1, 1)),
                )
                for i in range(nv):
                    factors = (axial[i, 0, v], cross[0, i, 0, v], cross[0, i, 1, v])
                    term = total([(0.5 * f) * s for f, s in zip(factors, spans)])
                    sums[i] = term if sums[i] is None else sums[i] + term
            values = [src[i, x, at] - sums[i] for i in range(nv)]
            for i in range(nv):
                res_out[0, i, x, at] = values[i]
            for i in range(nv):
                prov[i, x, at] = total([inv[i, j, x, at] * values[j] for j in range(nv)])
            return carry

        lax.fori_loop(0, planes, one, 0)

    def gather_facing(*targets):
        move_picks.wait()
        for other in range(sectors):
            facing_arrival(other).wait_recv()

        def pick(block, carry):
            for inner in range(GROUP):
                c = block * GROUP + inner
                at = picks[c, 0]
                part, column = at // columns, lax.rem(at, columns)
                for v in range(nv):
                    value = facing[part, v, pl.ds(column, 1)]
                    for target in targets:
                        target[v, pl.ds(c, 1)] = value
            return carry

        lax.fori_loop(0, groups, pick, 0)

    def forward_copy(g):
        return remote(
            leaving.at[:, columns_of(g)], entering.at[:, columns_of(g)],
            fw_send.at[g], fw_recv.at[g], slab=slab + 1,
        )

    def backward_copy(g):
        return remote(
            upd.at[:, columns_of(g)], following.at[:, columns_of(g)],
            bw_send.at[g], bw_recv.at[g], slab=slab - 1,
        )

    def sweep_up(g):
        at = columns_of(g)
        now = [entering[v, at] for v in range(nv)]
        for x in range(planes):
            if x == planes - 1:
                now = [now[v] - above[v, at] for v in range(nv)]
            now = [
                total([prov[i, x, at]] + [eff[i, j, x, at] * now[j] for j in range(nv)])
                for i in range(nv)
            ]
            for i in range(nv):
                prov[i, x, at] = now[i]

        @pl.when(has_high)
        def _():
            for i in range(nv):
                leaving[i, at] = now[i] + q[i, planes - 1, padded(g)]
            forward_copy(g).start()

    def sweep_down(g):
        at = columns_of(g)
        now = [following[v, at] for v in range(nv)]
        for x in reversed(range(planes)):
            now = [
                prov[i, x, at] - total([eff[i, j, x, at] * now[j] for j in range(nv)])
                for i in range(nv)
            ]
            if x == 0:
                for i in range(nv):
                    upd[i, at] = now[i]

                @pl.when(has_low)
                def _():
                    backward_copy(g).start()

            for i in range(nv):
                state_out[0, i, x, at] = q[i, x, padded(g)] + now[i]

    leads = both(rotor, is_first)
    inside = groups - 2

    def advance(step, carry):
        late = step >= 2 * inside
        fluxes = jnp.where(
            leads,
            jnp.logical_or(step < inside, both(late, lax.rem(step, 2) == 0)),
            step < groups,
        )
        flux_at = jnp.where(jnp.logical_and(leads, late), step // 2, step)
        sweep_at = jnp.where(
            leads, jnp.where(late, step // 2, step - inside), step - groups
        )

        @pl.when(fluxes)
        def _():
            @pl.when(flux_at == inside)
            def _():
                to_before.wait_recv()

            @pl.when(flux_at == inside + 1)
            def _():
                to_after.wait_recv()

            flux(lax.rem(flux_at + 1, groups))

        @pl.when(jnp.logical_not(fluxes))
        def _():
            g = lax.rem(sweep_at + 1, groups)

            @pl.when(sweep_at == 0)
            def _():
                @pl.when(has_high)
                def _():
                    to_low.wait_recv()
                    to_high.start()

                pl.when(rotor_top)(functools.partial(gather_facing, above))
                pl.when(stator_foot)(functools.partial(gather_facing, entering, below))

            @pl.when(has_low)
            def _():
                forward_copy(g).wait_recv()

            sweep_up(g)

            @pl.when(is_last)
            def _():
                sweep_down(g)

        return carry

    lax.fori_loop(0, 2 * groups, advance, 0)

    @pl.when(has_low)
    def _():
        to_high.wait_recv()

    for i in range(nv):
        res_out[0, i, 0] = res_out[0, i, 0] + total(
            [(0.5 * axial[i, 0, j]) * below[j] for j in range(nv)]
        )
    for i in range(nv):
        res_out[0, i, planes - 1] = res_out[0, i, planes - 1] - total(
            [(0.5 * axial[i, 0, j]) * above[j] for j in range(nv)]
        )

    to_after.wait_send()
    to_before.wait_send()

    @pl.when(has_high)
    def _():
        to_high.wait_send()

    @pl.when(has_low)
    def _():
        to_low.wait_send()

    @pl.when(on_plane)
    def _():
        for other in range(sectors):
            facing_copy(0, other).wait_send()

    @pl.when(has_high)
    def _():
        def back(step, carry):
            g = lax.rem(step + 1, groups)
            backward_copy(g).wait_recv()
            sweep_down(g)
            return carry

        lax.fori_loop(0, groups, back, 0)

    def finish(g, carry):
        @pl.when(has_high)
        def _():
            forward_copy(g).wait_send()

        @pl.when(has_low)
        def _():
            backward_copy(g).wait_send()

        return carry

    lax.fori_loop(0, groups, finish, 0)


def write_out(res_in, state_in, res_out, state_out, sems):
    first = pltpu.make_async_copy(res_in, res_out, sems.at[0])
    second = pltpu.make_async_copy(state_in, state_out, sems.at[1])
    first.start()
    second.start()
    first.wait()
    second.wait()


def per_device(state, source, diag_inverse, jac_axial, jac_cross, owner):
    _, nv, planes, columns, cells = state.shape
    sectors = lax.axis_size("sector")
    slabs = lax.axis_size("slab")
    groups = columns // GROUP

    def vmem(*shape):
        return pltpu.VMEM(shape, jnp.float32)

    dma = pltpu.SemaphoreType.DMA
    field = (nv, planes, columns, cells)
    plane = (nv, columns, cells)
    outside = pl.BlockSpec(memory_space=pltpu.HBM)
    inside = pl.BlockSpec(memory_space=pltpu.VMEM)
    residual, new_state = pl.pallas_call(
        functools.partial(kernel, sectors, slabs),
        out_shape=[vmem(*state.shape)] * 2,
        in_specs=[outside] * 6,
        out_specs=[inside] * 2,
        scratch_shapes=[
            pltpu.SMEM((nv, 1, nv), jnp.float32),
            pltpu.SMEM((1, nv, 2, nv), jnp.float32),
            pltpu.VMEM((1, owner.shape[0]), jnp.int32),
            pltpu.VMEM((columns, 128), jnp.int32),
            pltpu.SMEM((columns, 128), jnp.int32),
            vmem(nv, planes, columns + 2 * PAD, cells),
            vmem(*field),
            vmem(nv, *field),
            vmem(nv, *field),
            vmem(*field),
            vmem(*plane),
            vmem(*plane),
            vmem(sectors, *plane),
            vmem(*plane),
            vmem(*plane),
            vmem(*plane),
            vmem(*plane),
            dma((7,)),
            dma((2,)), dma((2,)), dma((2,)), dma((2,)),
            dma((sectors,)), dma((sectors,)),
            dma((groups,)), dma((groups,)), dma((groups,)), dma((groups,)),
            pltpu.SemaphoreType.REGULAR,
        ],
        compiler_params=pltpu.CompilerParams(collective_id=0, has_side_effects=True),
    )(state, source, diag_inverse, jnp.swapaxes(jac_axial, 0, 1),
        jnp.swapaxes(jac_cross, 1, 2), owner[None])
    return pl.pallas_call(
        write_out,
        out_shape=[jax.ShapeDtypeStruct(state.shape, jnp.float32)] * 2,
        in_specs=[inside] * 2,
        out_specs=[outside] * 2,
        scratch_shapes=[dma((2,))],
        compiler_params=pltpu.CompilerParams(vmem_limit_bytes=1 << 20),
    )(
        pltpu.with_memory_space_constraint(residual, pltpu.VMEM),
        pltpu.with_memory_space_constraint(new_state, pltpu.VMEM),
    )


def solution(mesh):
    return jax.shard_map(
        per_device,
        mesh=mesh,
        in_specs=(
            P("row", None, "slab", "sector", None),
            P("row", None, "slab", "sector", None),
            P("row", None, None, "slab", "sector", None),
            P("row", None, None),
            P("row", None, None, None),
            P(),
        ),
        out_specs=(P("row", None, "slab", "sector", None), P("row", None, "slab", "sector", None)),
        check_vma=False,
    )
```

```python
import functools

import jax
import jax.numpy as jnp
from jax import lax
from jax.experimental import pallas as pl
from jax.experimental.pallas import tpu as pltpu
from jax.sharding import PartitionSpec as P

MESH = pl.DeviceIdType.MESH
PAD = 8
GROUP = 8


def total(terms):
    while len(terms) > 1:
        pairs = [a + b for a, b in zip(terms[::2], terms[1::2])]
        if len(terms) % 2:
            pairs.append(terms[-1])
        terms = pairs
    return terms[0]


def both(*conditions):
    return functools.reduce(jnp.logical_and, conditions)


def kernel(
    sectors, slabs,
    state, source, inverse, axial_in, cross_in, owner_in,
    res_out, state_out,
    axial, cross, owner, picks_wide, picks,
    q, halo, src, inv, eff, prov, below, above, facing, entering, following, leaving, upd,
    local_sem, ax_send, ax_recv, se_send, se_recv,
    if_send, if_recv, fw_send, fw_recv, bw_send, bw_recv, sectors_in,
):
    nv, planes, columns, cells = src.shape
    groups = columns // GROUP
    row = lax.axis_index("row")
    sector = lax.axis_index("sector")
    slab = lax.axis_index("slab")
    rotor, stator = row == 0, row == 1
    has_low = slab > 0
    has_high = slab < slabs - 1
    is_first, is_last = slab == 0, slab == slabs - 1
    middle = both(has_low, has_high)
    outer = jnp.logical_or(is_first, is_last)
    rotor_top = both(rotor, is_last)
    stator_foot = both(stator, is_first)
    on_plane = jnp.logical_or(rotor_top, stator_foot)
    after = lax.rem(sector + 1, sectors)
    before = lax.rem(sector + sectors - 1, sectors)
    facing_slab = jnp.where(row == 0, 0, slabs - 1)
    body = pl.ds(PAD, columns)

    load_state = pltpu.make_async_copy(state.at[0], q.at[:, :, body], local_sem.at[0])
    load_state.start()
    load_axial = pltpu.make_async_copy(axial_in, axial, local_sem.at[4])
    load_axial.start()
    load_inverse = pltpu.make_async_copy(inverse.at[0], inv, local_sem.at[2])
    load_inverse.start()
    load_cross = pltpu.make_async_copy(cross_in, cross, local_sem.at[5])
    load_cross.start()
    load_owner = pltpu.make_async_copy(owner_in, owner, local_sem.at[3])
    load_owner.start()
    load_source = pltpu.make_async_copy(source.at[0], src, local_sem.at[1])
    load_source.start()

    barrier = pltpu.get_barrier_semaphore()

    def greet(**where):
        pl.semaphore_signal(barrier, inc=1, device_id=where, device_id_type=MESH)

    @pl.when(on_plane)
    def _():
        for other in range(sectors):
            greet(row=1 - row, sector=other, slab=facing_slab)

    @pl.when(has_high)
    def _():
        greet(slab=slab + 1)

    @pl.when(jnp.logical_or(stator, outer))
    def _():
        greet(sector=after)
        greet(sector=before)

    @pl.when(both(rotor, middle))
    def _():
        greet(row=1, sector=after)
        greet(row=1, sector=before)
        greet(row=1)

    peers = (
        has_low.astype(jnp.int32)
        + jnp.where(jnp.logical_or(stator, outer), 2, 0)
        + jnp.where(both(stator, middle), 3, 0)
        + jnp.where(on_plane, sectors, 0)
    )

    zero_plane = jnp.zeros((nv, columns, cells), jnp.float32)
    zero_columns = jnp.zeros((nv, planes, PAD, cells), jnp.float32)
    q[:, :, pl.ds(0, PAD)] = zero_columns
    q[:, :, pl.ds(PAD + columns, PAD)] = zero_columns

    @pl.when(is_first)
    def _():
        entering[...] = zero_plane
        below[...] = zero_plane

    @pl.when(is_last)
    def _():
        following[...] = zero_plane
        above[...] = zero_plane

    move_picks = pltpu.make_async_copy(picks_wide, picks, local_sem.at[6])
    load_owner.wait()

    @pl.when(on_plane)
    def _():
        shape = (columns, owner.shape[1])
        ids = sector * columns + lax.broadcasted_iota(jnp.int32, shape, 0)
        everyone = lax.broadcasted_iota(jnp.int32, shape, 1)
        owners = jnp.broadcast_to(owner[...], shape)
        is_rotor = jnp.broadcast_to(row, shape) == 0
        hits = jnp.where(is_rotor, everyone, owners) == ids
        found = jnp.sum(
            jnp.where(hits, jnp.where(is_rotor, owners, everyone), 0), axis=1, keepdims=True
        )
        found = jnp.minimum(found, owner.shape[1] - 1)
        picks_wide[...] = jnp.broadcast_to(found, picks_wide.shape)
        move_picks.start()

    def remote(source_ref, target_ref, send, recv, **where):
        return pltpu.make_async_remote_copy(
            src_ref=source_ref, dst_ref=target_ref, send_sem=send, recv_sem=recv,
            device_id=where, device_id_type=MESH,
        )

    def facing_copy(plane_at, other):
        return remote(
            q.at[:, plane_at, body], facing.at[sector], if_send.at[other], if_recv.at[sector],
            row=1 - row, sector=other, slab=facing_slab,
        )

    def facing_arrival(other):
        return remote(
            q.at[:, 0, body], facing.at[other], if_send.at[other], if_recv.at[other],
            row=1 - row, sector=other, slab=facing_slab,
        )

    to_after = remote(
        q.at[:, :, pl.ds(PAD + columns - 1, 1)], halo.at[0],
        se_send.at[0], se_recv.at[0], sector=after,
    )
    to_before = remote(
        q.at[:, :, pl.ds(PAD, 1)], halo.at[1],
        se_send.at[1], se_recv.at[1], sector=before,
    )

    def halo_arrival(side):
        return remote(
            q.at[:, :, pl.ds(PAD, 1)], halo.at[side],
            se_send.at[side], se_recv.at[side], sector=before,
        )
    to_high = remote(
        q.at[:, planes - 1, body], below, ax_send.at[0], ax_recv.at[0], slab=slab + 1
    )
    to_low = remote(
        q.at[:, 0, body], above, ax_send.at[1], ax_recv.at[1], slab=slab - 1
    )

    at_start = sector == 0

    def open_up():
        pl.semaphore_wait(barrier, peers)

        @pl.when(has_low)
        def _():
            to_low.start()

        @pl.when(rotor_top)
        def _():
            for other in range(sectors):
                facing_copy(planes - 1, other).start()

        @pl.when(stator_foot)
        def _():
            for other in range(sectors):
                facing_copy(0, other).start()

        @pl.when(both(stator, middle))
        def _():
            pl.semaphore_signal(
                sectors_in, inc=1, device_id=dict(row=0), device_id_type=MESH
            )

    def meet_sectors():
        @pl.when(both(rotor, middle))
        def _():
            pl.semaphore_wait(sectors_in, 1)

        to_after.start()
        to_before.start()

    def columns_of(g):
        return pl.ds(pl.multiple_of(g * GROUP, GROUP), GROUP)

    def padded(g):
        return pl.ds(pl.multiple_of(PAD + g * GROUP, GROUP), GROUP)

    lane = lax.broadcasted_iota(jnp.int32, (columns, cells), 1)
    no_cells = jnp.zeros((columns, cells), jnp.float32)

    def effective(x, carry):
        for i in range(nv):
            blocks = [inv[i, j, x] for j in range(nv)]
            for k in range(nv):
                eff[i, k, x] = total([blocks[j] * (0.5 * axial[j, 0, k]) for j in range(nv)])
        return carry

    def flux(x, carry):
        higher = jnp.minimum(x + 1, planes - 1)
        lower = jnp.maximum(x - 1, 0)
        sums = [None] * nv
        for v in range(nv):
            here = q[v, x, body]
            spans = (
                jnp.where(x == planes - 1, no_cells, q[v, higher, body])
                - jnp.where(x == 0, no_cells, q[v, lower, body]),
                q[v, x, pl.ds(PAD + 1, columns)] - q[v, x, pl.ds(PAD - 1, columns)],
                jnp.where(lane == cells - 1, 0.0, pltpu.roll(here, cells - 1, 1))
                - jnp.where(lane == 0, 0.0, pltpu.roll(here, 1, 1)),
            )
            for i in range(nv):
                factors = (axial[i, 0, v], cross[0, i, 0, v], cross[0, i, 1, v])
                term = total([f * s for f, s in zip(factors, spans)])
                sums[i] = term if sums[i] is None else sums[i] + term
        values = [src[i, x] - 0.5 * sums[i] for i in range(nv)]
        for i in range(nv):
            res_out[0, i, x] = values[i]
        for i in range(nv):
            prov[i, x] = total([inv[i, j, x] * values[j] for j in range(nv)])
        return carry

    def local_work():
        load_axial.wait()
        load_inverse.wait()
        lax.fori_loop(0, planes, effective, 0)
        load_cross.wait()
        load_source.wait()
        lax.fori_loop(0, planes, flux, 0)

    early = jnp.logical_or(jnp.logical_not(at_start), both(rotor, middle))
    opens_at = jnp.where(early, 0, 2)
    meets_at = jnp.where(at_start, 2, 0)
    load_state.wait()

    def prepare(step, carry):
        pl.when(step == opens_at)(open_up)
        pl.when(step == meets_at)(meet_sectors)
        pl.when(step == 1)(local_work)
        return carry

    lax.fori_loop(0, 3, prepare, 0)
    place = lax.broadcasted_iota(jnp.int32, (GROUP, cells), 0)

    def mend(side):
        halo_arrival(side).wait_recv()
        at = columns_of(side * (groups - 1))
        touched = place == side * (GROUP - 1)
        scale = jnp.where(side == 0, 0.5, -0.5)

        def one(x, carry):
            outside = [
                jnp.broadcast_to(halo[side, v, x], (GROUP, cells)) for v in range(nv)
            ]
            change = [
                jnp.where(
                    touched,
                    scale * total([cross[0, i, 0, v] * outside[v] for v in range(nv)]),
                    0.0,
                )
                for i in range(nv)
            ]
            for i in range(nv):
                res_out[0, i, x, at] = res_out[0, i, x, at] + change[i]
            for i in range(nv):
                prov[i, x, at] = prov[i, x, at] + total(
                    [inv[i, j, x, at] * change[j] for j in range(nv)]
                )
            return carry

        lax.fori_loop(0, planes, one, 0)

    def gather_facing(*targets):
        move_picks.wait()
        for other in range(sectors):
            facing_arrival(other).wait_recv()

        def pick(block, carry):
            for inner in range(GROUP):
                c = block * GROUP + inner
                at = picks[c, 0]
                part, column = at // columns, lax.rem(at, columns)
                for v in range(nv):
                    value = facing[part, v, pl.ds(column, 1)]
                    for target in targets:
                        target[v, pl.ds(c, 1)] = value
            return carry

        lax.fori_loop(0, groups, pick, 0)

    def forward_copy(g):
        return remote(
            leaving.at[:, columns_of(g)], entering.at[:, columns_of(g)],
            fw_send.at[g], fw_recv.at[g], slab=slab + 1,
        )

    def backward_copy(g):
        return remote(
            upd.at[:, columns_of(g)], following.at[:, columns_of(g)],
            bw_send.at[g], bw_recv.at[g], slab=slab - 1,
        )

    def sweep_up(g):
        at = columns_of(g)
        now = [entering[v, at] for v in range(nv)]
        for x in range(planes):
            if x == planes - 1:
                now = [now[v] - above[v, at] for v in range(nv)]
            now = [
                total([prov[i, x, at]] + [eff[i, j, x, at] * now[j] for j in range(nv)])
                for i in range(nv)
            ]
            for i in range(nv):
                prov[i, x, at] = now[i]

        @pl.when(has_high)
        def _():
            for i in range(nv):
                leaving[i, at] = now[i] + q[i, planes - 1, padded(g)]
            forward_copy(g).start()

    def sweep_down(g):
        at = columns_of(g)
        now = [following[v, at] for v in range(nv)]
        for x in reversed(range(planes)):
            now = [
                prov[i, x, at] - total([eff[i, j, x, at] * now[j] for j in range(nv)])
                for i in range(nv)
            ]
            if x == 0:
                for i in range(nv):
                    upd[i, at] = now[i]

                @pl.when(has_low)
                def _():
                    backward_copy(g).start()

            for i in range(nv):
                state_out[0, i, x, at] = q[i, x, padded(g)] + now[i]

    leads = both(rotor, slab <= 1)
    inside = groups - 2

    def advance(step, carry):
        mends = jnp.where(
            leads, jnp.logical_or(step == inside, step == groups), step < 2
        )
        side = jnp.where(step == jnp.where(leads, inside, 0), 1, 0)
        sweep_at = jnp.where(
            leads, step - (step > inside).astype(jnp.int32) - (step > groups).astype(jnp.int32),
            step - 2,
        )

        @pl.when(mends)
        def _():
            mend(side)

        @pl.when(jnp.logical_not(mends))
        def _():
            g = lax.rem(sweep_at + 1, groups)

            @pl.when(sweep_at == 0)
            def _():
                @pl.when(has_high)
                def _():
                    to_low.wait_recv()
                    to_high.start()

                pl.when(rotor_top)(functools.partial(gather_facing, above))
                pl.when(stator_foot)(functools.partial(gather_facing, entering, below))

            @pl.when(has_low)
            def _():
                forward_copy(g).wait_recv()

            sweep_up(g)

            @pl.when(is_last)
            def _():
                sweep_down(g)

        return carry

    lax.fori_loop(0, groups + 2, advance, 0)

    @pl.when(has_low)
    def _():
        to_high.wait_recv()

    for i in range(nv):
        res_out[0, i, 0] = res_out[0, i, 0] + total(
            [(0.5 * axial[i, 0, j]) * below[j] for j in range(nv)]
        )
    for i in range(nv):
        res_out[0, i, planes - 1] = res_out[0, i, planes - 1] - total(
            [(0.5 * axial[i, 0, j]) * above[j] for j in range(nv)]
        )

    to_after.wait_send()
    to_before.wait_send()

    @pl.when(has_high)
    def _():
        to_high.wait_send()

    @pl.when(has_low)
    def _():
        to_low.wait_send()

    @pl.when(on_plane)
    def _():
        for other in range(sectors):
            facing_copy(0, other).wait_send()

    @pl.when(has_high)
    def _():
        def back(step, carry):
            g = lax.rem(step + 1, groups)
            backward_copy(g).wait_recv()
            sweep_down(g)
            return carry

        lax.fori_loop(0, groups, back, 0)

    def finish(g, carry):
        @pl.when(has_high)
        def _():
            forward_copy(g).wait_send()

        @pl.when(has_low)
        def _():
            backward_copy(g).wait_send()

        return carry

    lax.fori_loop(0, groups, finish, 0)


def write_out(res_in, state_in, res_out, state_out, sems):
    first = pltpu.make_async_copy(res_in, res_out, sems.at[0])
    second = pltpu.make_async_copy(state_in, state_out, sems.at[1])
    first.start()
    second.start()
    first.wait()
    second.wait()


def per_device(state, source, diag_inverse, jac_axial, jac_cross, owner):
    _, nv, planes, columns, cells = state.shape
    sectors = lax.axis_size("sector")
    slabs = lax.axis_size("slab")
    groups = columns // GROUP

    def vmem(*shape):
        return pltpu.VMEM(shape, jnp.float32)

    dma = pltpu.SemaphoreType.DMA
    field = (nv, planes, columns, cells)
    plane = (nv, columns, cells)
    outside = pl.BlockSpec(memory_space=pltpu.HBM)
    inside = pl.BlockSpec(memory_space=pltpu.VMEM)
    residual, new_state = pl.pallas_call(
        functools.partial(kernel, sectors, slabs),
        out_shape=[vmem(*state.shape)] * 2,
        in_specs=[outside] * 6,
        out_specs=[inside] * 2,
        scratch_shapes=[
            pltpu.SMEM((nv, 1, nv), jnp.float32),
            pltpu.SMEM((1, nv, 2, nv), jnp.float32),
            pltpu.VMEM((1, owner.shape[0]), jnp.int32),
            pltpu.VMEM((columns, 128), jnp.int32),
            pltpu.SMEM((columns, 128), jnp.int32),
            vmem(nv, planes, columns + 2 * PAD, cells),
            vmem(2, nv, planes, 1, cells),
            vmem(*field),
            vmem(nv, *field),
            vmem(nv, *field),
            vmem(*field),
            vmem(*plane),
            vmem(*plane),
            vmem(sectors, *plane),
            vmem(*plane),
            vmem(*plane),
            vmem(*plane),
            vmem(*plane),
            dma((7,)),
            dma((2,)), dma((2,)), dma((2,)), dma((2,)),
            dma((sectors,)), dma((sectors,)),
            dma((groups,)), dma((groups,)), dma((groups,)), dma((groups,)),
            pltpu.SemaphoreType.REGULAR,
        ],
        compiler_params=pltpu.CompilerParams(collective_id=0, has_side_effects=True),
    )(state, source, diag_inverse, jnp.swapaxes(jac_axial, 0, 1),
        jnp.swapaxes(jac_cross, 1, 2), owner[None])
    return pl.pallas_call(
        write_out,
        out_shape=[jax.ShapeDtypeStruct(state.shape, jnp.float32)] * 2,
        in_specs=[inside] * 2,
        out_specs=[outside] * 2,
        scratch_shapes=[dma((2,))],
        compiler_params=pltpu.CompilerParams(vmem_limit_bytes=1 << 20),
    )(
        pltpu.with_memory_space_constraint(residual, pltpu.VMEM),
        pltpu.with_memory_space_constraint(new_state, pltpu.VMEM),
    )


def solution(mesh):
    return jax.shard_map(
        per_device,
        mesh=mesh,
        in_specs=(
            P("row", None, "slab", "sector", None),
            P("row", None, "slab", "sector", None),
            P("row", None, None, "slab", "sector", None),
            P("row", None, None),
            P("row", None, None, None),
            P(),
        ),
        out_specs=(P("row", None, "slab", "sector", None), P("row", None, "slab", "sector", None)),
        check_vma=False,
    )
```

```python
import functools

import jax
import jax.numpy as jnp
from jax import lax
from jax.experimental import pallas as pl
from jax.experimental.pallas import tpu as pltpu
from jax.sharding import PartitionSpec as P

MESH = pl.DeviceIdType.MESH
PAD = 8
GROUP = 8


def total(terms):
    while len(terms) > 1:
        pairs = [a + b for a, b in zip(terms[::2], terms[1::2])]
        if len(terms) % 2:
            pairs.append(terms[-1])
        terms = pairs
    return terms[0]


def both(*conditions):
    return functools.reduce(jnp.logical_and, conditions)


def kernel(
    sectors, slabs,
    state, source, inverse, axial_in, cross_in, owner_in,
    res_out, state_out,
    axial, cross, owner, picks_wide, picks,
    q, halo, src, inv, eff, prov, below, above, facing, entering, following, leaving, upd,
    base, mats_out, mats_in, powers, trial,
    local_sem, ax_send, ax_recv, se_send, se_recv,
    if_send, if_recv, fw_send, fw_recv, bw_send, bw_recv,
    skip_send, base_recv, mat_send, mat_recv, sectors_in,
):
    nv, planes, columns, cells = src.shape
    groups = columns // GROUP
    row = lax.axis_index("row")
    sector = lax.axis_index("sector")
    slab = lax.axis_index("slab")
    rotor, stator = row == 0, row == 1
    has_low = slab > 0
    has_high = slab < slabs - 1
    is_first, is_last = slab == 0, slab == slabs - 1
    is_second, is_third = slab == 1, slab == 2
    is_turn = slab == slabs - 2
    middle = both(has_low, has_high)
    outer = jnp.logical_or(is_first, is_last)
    rotor_top = both(rotor, is_last)
    stator_foot = both(stator, is_first)
    on_plane = jnp.logical_or(rotor_top, stator_foot)
    after = lax.rem(sector + 1, sectors)
    before = lax.rem(sector + sectors - 1, sectors)
    facing_slab = jnp.where(row == 0, 0, slabs - 1)
    body = pl.ds(PAD, columns)

    load_state = pltpu.make_async_copy(state.at[0], q.at[:, :, body], local_sem.at[0])
    load_state.start()
    load_axial = pltpu.make_async_copy(axial_in, axial, local_sem.at[4])
    load_axial.start()
    load_inverse = pltpu.make_async_copy(inverse.at[0], inv, local_sem.at[2])
    load_inverse.start()
    load_cross = pltpu.make_async_copy(cross_in, cross, local_sem.at[5])
    load_cross.start()
    load_owner = pltpu.make_async_copy(owner_in, owner, local_sem.at[3])
    load_owner.start()
    load_source = pltpu.make_async_copy(source.at[0], src, local_sem.at[1])
    load_source.start()

    barrier = pltpu.get_barrier_semaphore()

    def greet(**where):
        pl.semaphore_signal(barrier, inc=1, device_id=where, device_id_type=MESH)

    @pl.when(on_plane)
    def _():
        for other in range(sectors):
            greet(row=1 - row, sector=other, slab=facing_slab)

    @pl.when(has_high)
    def _():
        greet(slab=slab + 1)

    @pl.when(jnp.logical_or(stator, outer))
    def _():
        greet(sector=after)
        greet(sector=before)

    @pl.when(both(rotor, middle))
    def _():
        greet(row=1, sector=after)
        greet(row=1, sector=before)
        greet(row=1)

    peers = (
        has_low.astype(jnp.int32)
        + jnp.where(jnp.logical_or(stator, outer), 2, 0)
        + jnp.where(both(stator, middle), 3, 0)
        + jnp.where(on_plane, sectors, 0)
    )

    zero_plane = jnp.zeros((nv, columns, cells), jnp.float32)
    zero_columns = jnp.zeros((nv, planes, PAD, cells), jnp.float32)
    q[:, :, pl.ds(0, PAD)] = zero_columns
    q[:, :, pl.ds(PAD + columns, PAD)] = zero_columns

    @pl.when(is_first)
    def _():
        entering[...] = zero_plane
        below[...] = zero_plane

    @pl.when(is_last)
    def _():
        following[...] = zero_plane
        above[...] = zero_plane

    move_picks = pltpu.make_async_copy(picks_wide, picks, local_sem.at[6])
    load_owner.wait()

    @pl.when(on_plane)
    def _():
        shape = (columns, owner.shape[1])
        ids = sector * columns + lax.broadcasted_iota(jnp.int32, shape, 0)
        everyone = lax.broadcasted_iota(jnp.int32, shape, 1)
        owners = jnp.broadcast_to(owner[...], shape)
        is_rotor = jnp.broadcast_to(row, shape) == 0
        hits = jnp.where(is_rotor, everyone, owners) == ids
        found = jnp.sum(
            jnp.where(hits, jnp.where(is_rotor, owners, everyone), 0), axis=1, keepdims=True
        )
        found = jnp.minimum(found, owner.shape[1] - 1)
        picks_wide[...] = jnp.broadcast_to(found, picks_wide.shape)
        move_picks.start()

    def remote(source_ref, target_ref, send, recv, **where):
        return pltpu.make_async_remote_copy(
            src_ref=source_ref, dst_ref=target_ref, send_sem=send, recv_sem=recv,
            device_id=where, device_id_type=MESH,
        )

    def facing_copy(plane_at, other):
        return remote(
            q.at[:, plane_at, body], facing.at[sector], if_send.at[other], if_recv.at[sector],
            row=1 - row, sector=other, slab=facing_slab,
        )

    def facing_arrival(other):
        return remote(
            q.at[:, 0, body], facing.at[other], if_send.at[other], if_recv.at[other],
            row=1 - row, sector=other, slab=facing_slab,
        )

    to_after = remote(
        q.at[:, :, pl.ds(PAD + columns - 1, 1)], halo.at[0],
        se_send.at[0], se_recv.at[0], sector=after,
    )
    to_before = remote(
        q.at[:, :, pl.ds(PAD, 1)], halo.at[1],
        se_send.at[1], se_recv.at[1], sector=before,
    )

    def halo_arrival(side):
        return remote(
            q.at[:, :, pl.ds(PAD, 1)], halo.at[side],
            se_send.at[side], se_recv.at[side], sector=before,
        )
    to_high = remote(
        q.at[:, planes - 1, body], below, ax_send.at[0], ax_recv.at[0], slab=slab + 1
    )
    to_low = remote(
        q.at[:, 0, body], above, ax_send.at[1], ax_recv.at[1], slab=slab - 1
    )

    at_start = sector == 0

    def open_up():
        pl.semaphore_wait(barrier, peers)

        @pl.when(has_low)
        def _():
            to_low.start()

        @pl.when(rotor_top)
        def _():
            for other in range(sectors):
                facing_copy(planes - 1, other).start()

        @pl.when(stator_foot)
        def _():
            for other in range(sectors):
                facing_copy(0, other).start()

        @pl.when(both(stator, middle))
        def _():
            pl.semaphore_signal(
                sectors_in, inc=1, device_id=dict(row=0), device_id_type=MESH
            )

    def meet_sectors():
        @pl.when(both(rotor, middle))
        def _():
            pl.semaphore_wait(sectors_in, 1)

        to_after.start()
        to_before.start()

    def columns_of(g):
        return pl.ds(pl.multiple_of(g * GROUP, GROUP), GROUP)

    def padded(g):
        return pl.ds(pl.multiple_of(PAD + g * GROUP, GROUP), GROUP)

    lane = lax.broadcasted_iota(jnp.int32, (columns, cells), 1)
    no_cells = jnp.zeros((columns, cells), jnp.float32)

    def effective(x, carry):
        for i in range(nv):
            blocks = [inv[i, j, x] for j in range(nv)]
            for k in range(nv):
                eff[i, k, x] = total([blocks[j] * (0.5 * axial[j, 0, k]) for j in range(nv)])
        return carry

    def flux(x, carry):
        higher = jnp.minimum(x + 1, planes - 1)
        lower = jnp.maximum(x - 1, 0)
        sums = [None] * nv
        for v in range(nv):
            here = q[v, x, body]
            spans = (
                jnp.where(x == planes - 1, no_cells, q[v, higher, body])
                - jnp.where(x == 0, no_cells, q[v, lower, body]),
                q[v, x, pl.ds(PAD + 1, columns)] - q[v, x, pl.ds(PAD - 1, columns)],
                jnp.where(lane == cells - 1, 0.0, pltpu.roll(here, cells - 1, 1))
                - jnp.where(lane == 0, 0.0, pltpu.roll(here, 1, 1)),
            )
            for i in range(nv):
                factors = (axial[i, 0, v], cross[0, i, 0, v], cross[0, i, 1, v])
                term = total([f * s for f, s in zip(factors, spans)])
                sums[i] = term if sums[i] is None else sums[i] + term
        values = [src[i, x] - 0.5 * sums[i] for i in range(nv)]
        for i in range(nv):
            res_out[0, i, x] = values[i]
        for i in range(nv):
            prov[i, x] = total([inv[i, j, x] * values[j] for j in range(nv)])
        return carry

    def local_work():
        load_axial.wait()
        load_inverse.wait()
        lax.fori_loop(0, planes, effective, 0)
        load_cross.wait()
        load_source.wait()
        lax.fori_loop(0, planes, flux, 0)

    early = jnp.logical_or(jnp.logical_not(at_start), both(rotor, middle))
    opens_at = jnp.where(early, 0, 2)
    meets_at = jnp.where(at_start, 2, 0)
    load_state.wait()

    def prepare(step, carry):
        pl.when(step == opens_at)(open_up)
        pl.when(step == meets_at)(meet_sectors)
        pl.when(step == 1)(local_work)
        return carry

    lax.fori_loop(0, 3, prepare, 0)
    place = lax.broadcasted_iota(jnp.int32, (GROUP, cells), 0)

    def mend(side):
        halo_arrival(side).wait_recv()
        at = columns_of(side * (groups - 1))
        touched = place == side * (GROUP - 1)
        scale = jnp.where(side == 0, 0.5, -0.5)

        def one(x, carry):
            outside = [
                jnp.broadcast_to(halo[side, v, x], (GROUP, cells)) for v in range(nv)
            ]
            change = [
                jnp.where(
                    touched,
                    scale * total([cross[0, i, 0, v] * outside[v] for v in range(nv)]),
                    0.0,
                )
                for i in range(nv)
            ]
            for i in range(nv):
                res_out[0, i, x, at] = res_out[0, i, x, at] + change[i]
            for i in range(nv):
                prov[i, x, at] = prov[i, x, at] + total(
                    [inv[i, j, x, at] * change[j] for j in range(nv)]
                )
            return carry

        lax.fori_loop(0, planes, one, 0)

    def gather_facing(*targets):
        move_picks.wait()
        for other in range(sectors):
            facing_arrival(other).wait_recv()

        def pick(block, carry):
            for inner in range(GROUP):
                c = block * GROUP + inner
                at = picks[c, 0]
                part, column = at // columns, lax.rem(at, columns)
                for v in range(nv):
                    value = facing[part, v, pl.ds(column, 1)]
                    for target in targets:
                        target[v, pl.ds(c, 1)] = value
            return carry

        lax.fori_loop(0, groups, pick, 0)

    def forward_copy(g):
        return remote(
            leaving.at[:, columns_of(g)], entering.at[:, columns_of(g)],
            fw_send.at[g], fw_recv.at[g], slab=slab + 1,
        )

    def backward_copy(g):
        return remote(
            upd.at[:, columns_of(g)], following.at[:, columns_of(g)],
            bw_send.at[g], bw_recv.at[g], slab=slab - 1,
        )

    def skip_copy(g):
        return remote(
            upd.at[:, columns_of(g)], following.at[:, columns_of(g)],
            skip_send.at[g], bw_recv.at[g], slab=0,
        )

    def base_copy(g):
        return remote(
            upd.at[:, columns_of(g)], base.at[:, columns_of(g)],
            bw_send.at[g], base_recv.at[g], slab=0,
        )

    def mat_copy(g):
        return remote(
            mats_out.at[:, :, columns_of(g)], mats_in.at[:, :, columns_of(g)],
            mat_send.at[g], mat_recv.at[g], slab=slab - 1,
        )

    def blocks_at(x, at):
        return [[eff[i, j, x, at] for j in range(nv)] for i in range(nv)]

    def times(left, right):
        return [
            [total([left[i][j] * right[j][k] for j in range(nv)]) for k in range(nv)]
            for i in range(nv)
        ]

    def pack(matrix):
        return tuple(matrix[i][k] for i in range(nv) for k in range(nv))

    def unpack(values):
        return [list(values[i * nv : i * nv + nv]) for i in range(nv)]

    def send_matrix(g, values):
        at = columns_of(g)
        matrix = unpack(values)
        for i in range(nv):
            for k in range(nv):
                mats_out[i, k, at] = matrix[i][k]
        mat_copy(g).start()

    def entry_to_update(step, carry):
        g = lax.rem(step + 1, groups)
        at = columns_of(g)
        first = blocks_at(0, at)
        for i in range(nv):
            for k in range(nv):
                powers[i, k, 0] = first[i][k]

        def up(x, values):
            product = times(blocks_at(x, at), unpack(values))
            for i in range(nv):
                for k in range(nv):
                    powers[i, k, x] = product[i][k]
            return pack(product)

        def down(step, values):
            x = planes - 2 - step
            product = times(blocks_at(x, at), unpack(values))
            return pack(
                [[powers[i, k, x] - product[i][k] for k in range(nv)] for i in range(nv)]
            )

        values = lax.fori_loop(1, planes, up, pack(first))
        send_matrix(g, lax.fori_loop(0, planes - 1, down, values))
        return carry

    def exit_to_update(step, carry):
        g = lax.rem(step + 1, groups)
        at = columns_of(g)

        def down(step, values):
            product = times(blocks_at(planes - 2 - step, at), unpack(values))
            return pack([[-value for value in line] for line in product])

        last = [[-value for value in line] for line in blocks_at(planes - 1, at)]
        send_matrix(g, lax.fori_loop(0, planes - 1, down, pack(last)))
        return carry

    @pl.when(is_last)
    def _():
        lax.fori_loop(0, groups, entry_to_update, 0)

    @pl.when(is_second)
    def _():
        lax.fori_loop(0, groups, exit_to_update, 0)

    def climb(g, now, keep):
        at = columns_of(g)
        for x in range(planes):
            if x == planes - 1:
                now = [now[v] - above[v, at] for v in range(nv)]
            now = [
                total([prov[i, x, at]] + [eff[i, j, x, at] * now[j] for j in range(nv)])
                for i in range(nv)
            ]
            for i in range(nv):
                keep(i, x, now[i])
        return now

    def sweep_up(g):
        at = columns_of(g)

        def keep(i, x, value):
            prov[i, x, at] = value

        now = climb(g, [entering[v, at] for v in range(nv)], keep)

        @pl.when(has_high)
        def _():
            for i in range(nv):
                leaving[i, at] = now[i] + q[i, planes - 1, padded(g)]
            forward_copy(g).start()

    def sweep_down(g, now, known, keep=None):
        at = columns_of(g)
        for x in reversed(range(planes)):
            now = [
                known(i, x) - total([eff[i, j, x, at] * now[j] for j in range(nv)])
                for i in range(nv)
            ]
            if keep is not None:
                keep(x, now)
        return now

    nothing = jnp.zeros((GROUP, cells), jnp.float32)

    def try_alone(g):
        def keep(i, x, value):
            trial[i, x] = value

        climb(g, [nothing] * nv, keep)
        now = sweep_down(g, [nothing] * nv, lambda i, x: trial[i, x])
        for i in range(nv):
            upd[i, columns_of(g)] = now[i]
        backward_copy(g).start()

    def applied(g, added, factor):
        at = columns_of(g)
        return [
            total([added[i, at]] + [mats_in[i, j, at] * factor[j, at] for j in range(nv)])
            for i in range(nv)
        ]

    leads = both(rotor, slab <= 1)
    inside = groups - 2

    def advance(step, carry):
        mends = jnp.where(
            leads, jnp.logical_or(step == inside, step == groups), step < 2
        )
        side = jnp.where(step == jnp.where(leads, inside, 0), 1, 0)
        sweep_at = jnp.where(
            leads, step - (step > inside).astype(jnp.int32) - (step > groups).astype(jnp.int32),
            step - 2,
        )

        @pl.when(mends)
        def _():
            mend(side)

        @pl.when(jnp.logical_not(mends))
        def _():
            g = lax.rem(sweep_at + 1, groups)

            @pl.when(sweep_at == 0)
            def _():
                @pl.when(has_high)
                def _():
                    to_low.wait_recv()
                    to_high.start()

                pl.when(rotor_top)(functools.partial(gather_facing, above))
                pl.when(stator_foot)(functools.partial(gather_facing, entering, below))

            pl.when(is_last)(functools.partial(try_alone, g))

            @pl.when(both(has_low, has_high))
            def _():
                forward_copy(g).wait_recv()

            pl.when(has_high)(functools.partial(sweep_up, g))

        return carry

    lax.fori_loop(0, groups + 2, advance, 0)

    @pl.when(is_second)
    def _():
        def ahead(step, carry):
            g = lax.rem(step + 1, groups)
            at = columns_of(g)
            now = sweep_down(g, [nothing] * nv, lambda i, x: prov[i, x, at])
            for i in range(nv):
                upd[i, at] = now[i]
            base_copy(g).start()
            return carry

        lax.fori_loop(0, groups, ahead, 0)

    @pl.when(has_low)
    def _():
        to_high.wait_recv()

    for i in range(nv):
        res_out[0, i, 0] = res_out[0, i, 0] + total(
            [(0.5 * axial[i, 0, j]) * below[j] for j in range(nv)]
        )
    for i in range(nv):
        res_out[0, i, planes - 1] = res_out[0, i, planes - 1] - total(
            [(0.5 * axial[i, 0, j]) * above[j] for j in range(nv)]
        )

    to_after.wait_send()
    to_before.wait_send()

    @pl.when(has_high)
    def _():
        to_high.wait_send()

    @pl.when(has_low)
    def _():
        to_low.wait_send()

    @pl.when(on_plane)
    def _():
        for other in range(sectors):
            facing_copy(0, other).wait_send()

    def back(step, carry):
        g = lax.rem(step + 1, groups)
        at = columns_of(g)

        @pl.when(is_last)
        def _():
            forward_copy(g).wait_recv()
            sweep_up(g)

        @pl.when(has_high)
        def _():
            backward_copy(g).wait_recv()

        @pl.when(is_turn)
        def _():
            mat_copy(g).wait_recv()
            now = applied(g, following, leaving)
            for i in range(nv):
                following[i, at] = now[i]

        @pl.when(is_first)
        def _():
            mat_copy(g).wait_recv()
            base_copy(g).wait_recv()
            now = applied(g, base, following)
            for i in range(nv):
                following[i, at] = now[i]

        def keep(x, now):
            if x == 0:
                @pl.when(both(slab >= 2, has_high))
                def _():
                    for i in range(nv):
                        upd[i, at] = now[i]
                    backward_copy(g).start()

                    @pl.when(is_third)
                    def _():
                        skip_copy(g).start()

            for i in range(nv):
                state_out[0, i, x, at] = q[i, x, padded(g)] + now[i]

        sweep_down(
            g, [following[v, at] for v in range(nv)], lambda i, x: prov[i, x, at], keep
        )
        return carry

    lax.fori_loop(0, groups, back, 0)

    def finish(g, carry):
        @pl.when(has_high)
        def _():
            forward_copy(g).wait_send()

        @pl.when(has_low)
        def _():
            backward_copy(g).wait_send()

        @pl.when(is_third)
        def _():
            skip_copy(g).wait_send()

        @pl.when(jnp.logical_or(is_last, is_second))
        def _():
            mat_copy(g).wait_send()

        return carry

    lax.fori_loop(0, groups, finish, 0)


def write_out(res_in, state_in, res_out, state_out, sems):
    first = pltpu.make_async_copy(res_in, res_out, sems.at[0])
    second = pltpu.make_async_copy(state_in, state_out, sems.at[1])
    first.start()
    second.start()
    first.wait()
    second.wait()


def per_device(state, source, diag_inverse, jac_axial, jac_cross, owner):
    _, nv, planes, columns, cells = state.shape
    sectors = lax.axis_size("sector")
    slabs = lax.axis_size("slab")
    groups = columns // GROUP

    def vmem(*shape):
        return pltpu.VMEM(shape, jnp.float32)

    dma = pltpu.SemaphoreType.DMA
    field = (nv, planes, columns, cells)
    plane = (nv, columns, cells)
    outside = pl.BlockSpec(memory_space=pltpu.HBM)
    inside = pl.BlockSpec(memory_space=pltpu.VMEM)
    residual, new_state = pl.pallas_call(
        functools.partial(kernel, sectors, slabs),
        out_shape=[vmem(*state.shape)] * 2,
        in_specs=[outside] * 6,
        out_specs=[inside] * 2,
        scratch_shapes=[
            pltpu.SMEM((nv, 1, nv), jnp.float32),
            pltpu.SMEM((1, nv, 2, nv), jnp.float32),
            pltpu.VMEM((1, owner.shape[0]), jnp.int32),
            pltpu.VMEM((columns, 128), jnp.int32),
            pltpu.SMEM((columns, 128), jnp.int32),
            vmem(nv, planes, columns + 2 * PAD, cells),
            vmem(2, nv, planes, 1, cells),
            vmem(*field),
            vmem(nv, *field),
            vmem(nv, *field),
            vmem(*field),
            vmem(*plane),
            vmem(*plane),
            vmem(sectors, *plane),
            vmem(*plane),
            vmem(*plane),
            vmem(*plane),
            vmem(*plane),
            vmem(*plane),
            vmem(nv, *plane),
            vmem(nv, *plane),
            vmem(nv, nv, planes, GROUP, cells),
            vmem(nv, planes, GROUP, cells),
            dma((7,)),
            dma((2,)), dma((2,)), dma((2,)), dma((2,)),
            dma((sectors,)), dma((sectors,)),
            dma((groups,)), dma((groups,)), dma((groups,)), dma((groups,)),
            dma((groups,)), dma((groups,)), dma((groups,)), dma((groups,)),
            pltpu.SemaphoreType.REGULAR,
        ],
        compiler_params=pltpu.CompilerParams(collective_id=0, has_side_effects=True),
    )(state, source, diag_inverse, jnp.swapaxes(jac_axial, 0, 1),
        jnp.swapaxes(jac_cross, 1, 2), owner[None])
    return pl.pallas_call(
        write_out,
        out_shape=[jax.ShapeDtypeStruct(state.shape, jnp.float32)] * 2,
        in_specs=[inside] * 2,
        out_specs=[outside] * 2,
        scratch_shapes=[dma((2,))],
        compiler_params=pltpu.CompilerParams(vmem_limit_bytes=1 << 20),
    )(
        pltpu.with_memory_space_constraint(residual, pltpu.VMEM),
        pltpu.with_memory_space_constraint(new_state, pltpu.VMEM),
    )


def solution(mesh):
    return jax.shard_map(
        per_device,
        mesh=mesh,
        in_specs=(
            P("row", None, "slab", "sector", None),
            P("row", None, "slab", "sector", None),
            P("row", None, None, "slab", "sector", None),
            P("row", None, None),
            P("row", None, None, None),
            P(),
        ),
        out_specs=(P("row", None, "slab", "sector", None), P("row", None, "slab", "sector", None)),
        check_vma=False,
    )
```

```python
import functools

import jax
import jax.numpy as jnp
from jax import lax
from jax.experimental import pallas as pl
from jax.experimental.pallas import tpu as pltpu
from jax.sharding import PartitionSpec as P

MESH = pl.DeviceIdType.MESH
PAD = 8
GROUP = 8


def total(terms):
    while len(terms) > 1:
        pairs = [a + b for a, b in zip(terms[::2], terms[1::2])]
        if len(terms) % 2:
            pairs.append(terms[-1])
        terms = pairs
    return terms[0]


def both(*conditions):
    return functools.reduce(jnp.logical_and, conditions)


def kernel(
    sectors, slabs,
    state, source, inverse, axial_in, cross_in, owner_in,
    res_out, state_out,
    axial, cross, owner, picks_wide, picks,
    q, halo, src, inv, eff, prov, below, above, facing, entering, following, leaving, upd,
    base, mats_out, mats_in, powers, trial,
    local_sem, ax_send, ax_recv, se_send, se_recv,
    if_send, if_recv, fw_send, fw_recv, bw_send, bw_recv,
    skip_send, base_recv, mat_send, mat_recv, low_send, low_recv, sectors_in, turn_free,
):
    nv, planes, columns, cells = src.shape
    groups = columns // GROUP
    row = lax.axis_index("row")
    sector = lax.axis_index("sector")
    slab = lax.axis_index("slab")
    rotor, stator = row == 0, row == 1
    has_low = slab > 0
    has_high = slab < slabs - 1
    is_first, is_last = slab == 0, slab == slabs - 1
    is_second, is_third = slab == 1, slab == 2
    is_turn = slab == slabs - 2
    middle = both(has_low, has_high)
    outer = jnp.logical_or(is_first, is_last)
    rotor_top = both(rotor, is_last)
    stator_foot = both(stator, is_first)
    on_plane = jnp.logical_or(rotor_top, stator_foot)
    after = lax.rem(sector + 1, sectors)
    before = lax.rem(sector + sectors - 1, sectors)
    facing_slab = jnp.where(row == 0, 0, slabs - 1)
    body = pl.ds(PAD, columns)

    def state_copy(first, count, at):
        part = pl.ds(first, count)
        return pltpu.make_async_copy(state.at[0, :, part], q.at[:, part, body], local_sem.at[at])

    load_low, load_high = state_copy(0, 1, 0), state_copy(planes - 1, 1, 7)
    load_state = state_copy(1, planes - 2, 8)
    load_low.start()
    load_high.start()
    load_state.start()
    load_axial = pltpu.make_async_copy(axial_in, axial, local_sem.at[4])
    load_axial.start()
    load_inverse = pltpu.make_async_copy(inverse.at[0], inv, local_sem.at[2])
    load_inverse.start()
    load_cross = pltpu.make_async_copy(cross_in, cross, local_sem.at[5])
    load_cross.start()
    load_owner = pltpu.make_async_copy(owner_in, owner, local_sem.at[3])
    load_owner.start()
    load_source = pltpu.make_async_copy(source.at[0], src, local_sem.at[1])
    load_source.start()

    barrier = pltpu.get_barrier_semaphore()

    def greet(**where):
        pl.semaphore_signal(barrier, inc=1, device_id=where, device_id_type=MESH)

    @pl.when(on_plane)
    def _():
        greet(row=1 - row, slab=facing_slab)
        for step in range(1, sectors):
            greet(sector=lax.rem(sector + step, sectors))

    @pl.when(has_high)
    def _():
        greet(slab=slab + 1)

    beside = both(jnp.logical_or(stator, outer), jnp.logical_not(on_plane))

    @pl.when(beside)
    def _():
        greet(sector=after)
        greet(sector=before)

    @pl.when(both(rotor, middle))
    def _():
        greet(row=1, sector=after)
        greet(row=1, sector=before)
        greet(row=1)

    @pl.when(both(stator, is_last))
    def _():
        greet(row=0)

    peers = (
        has_low.astype(jnp.int32)
        + rotor_top.astype(jnp.int32)
        + jnp.where(beside, 2, 0)
        + jnp.where(both(stator, middle), 3, 0)
        + jnp.where(on_plane, sectors, 0)
    )

    def remote(source_ref, target_ref, send, recv, **where):
        return pltpu.make_async_remote_copy(
            src_ref=source_ref, dst_ref=target_ref, send_sem=send, recv_sem=recv,
            device_id=where, device_id_type=MESH,
        )

    def columns_of(g):
        return pl.ds(pl.multiple_of(g * GROUP, GROUP), GROUP)

    def padded(g):
        return pl.ds(pl.multiple_of(PAD + g * GROUP, GROUP), GROUP)

    def facing_copy(plane_at):
        return remote(
            q.at[:, plane_at, body], facing.at[sector], if_send.at[0], if_recv.at[sector],
            row=1 - row, slab=facing_slab,
        )

    def facing_relay(step):
        return remote(
            facing.at[sector], facing.at[sector], if_send.at[step], if_recv.at[sector],
            sector=lax.rem(sector + step, sectors),
        )

    def facing_arrival(step):
        origin = lax.rem(sector + step, sectors)
        return remote(
            facing.at[origin], facing.at[origin], if_send.at[step], if_recv.at[origin],
            sector=origin,
        )

    to_after = remote(
        q.at[:, :, pl.ds(PAD + columns - 1, 1)], halo.at[0],
        se_send.at[0], se_recv.at[0], sector=after,
    )
    to_before = remote(
        q.at[:, :, pl.ds(PAD, 1)], halo.at[1],
        se_send.at[1], se_recv.at[1], sector=before,
    )

    def halo_arrival(side):
        return remote(
            q.at[:, :, pl.ds(PAD, 1)], halo.at[side],
            se_send.at[side], se_recv.at[side], sector=before,
        )
    to_high = remote(
        q.at[:, planes - 1, body], below, ax_send.at[0], ax_recv.at[0], slab=slab + 1
    )

    def low_copy(g):
        return remote(
            q.at[:, 0, padded(g)], above.at[:, columns_of(g)],
            low_send.at[g], low_recv.at[g], slab=slab - 1,
        )

    def clear():
        zero_plane = jnp.zeros((nv, columns, cells), jnp.float32)
        zero_columns = jnp.zeros((nv, planes, PAD, cells), jnp.float32)
        q[:, :, pl.ds(0, PAD)] = zero_columns
        q[:, :, pl.ds(PAD + columns, PAD)] = zero_columns

        @pl.when(is_first)
        def _():
            entering[...] = zero_plane
            below[...] = zero_plane

        @pl.when(is_last)
        def _():
            following[...] = zero_plane
            above[...] = zero_plane

    at_start = sector == 0

    def open_up():
        pl.semaphore_wait(barrier, peers)

        @pl.when(has_low)
        def _():
            for step in range(groups):
                low_copy((step + 1) % groups).start()

        @pl.when(rotor_top)
        def _():
            facing_copy(planes - 1).start()

        @pl.when(stator_foot)
        def _():
            facing_copy(0).start()

        @pl.when(both(stator, middle))
        def _():
            pl.semaphore_signal(
                sectors_in, inc=1, device_id=dict(row=0), device_id_type=MESH
            )

    def meet_sectors():
        @pl.when(both(rotor, middle))
        def _():
            pl.semaphore_wait(sectors_in, 1)

        to_after.start()
        to_before.start()

    lane = lax.broadcasted_iota(jnp.int32, (columns, cells), 1)
    no_cells = jnp.zeros((columns, cells), jnp.float32)

    def effective(x, carry):
        for i in range(nv):
            blocks = [inv[i, j, x] for j in range(nv)]
            for k in range(nv):
                eff[i, k, x] = total([blocks[j] * (0.5 * axial[j, 0, k]) for j in range(nv)])
        return carry

    def flux(x, carry):
        higher = jnp.minimum(x + 1, planes - 1)
        lower = jnp.maximum(x - 1, 0)
        sums = [None] * nv
        for v in range(nv):
            here = q[v, x, body]
            spans = (
                jnp.where(x == planes - 1, no_cells, q[v, higher, body])
                - jnp.where(x == 0, no_cells, q[v, lower, body]),
                q[v, x, pl.ds(PAD + 1, columns)] - q[v, x, pl.ds(PAD - 1, columns)],
                jnp.where(lane == cells - 1, 0.0, pltpu.roll(here, cells - 1, 1))
                - jnp.where(lane == 0, 0.0, pltpu.roll(here, 1, 1)),
            )
            for i in range(nv):
                factors = (axial[i, 0, v], cross[0, i, 0, v], cross[0, i, 1, v])
                term = total([f * s for f, s in zip(factors, spans)])
                sums[i] = term if sums[i] is None else sums[i] + term
        values = [src[i, x] - 0.5 * sums[i] for i in range(nv)]
        for i in range(nv):
            res_out[0, i, x] = values[i]
        for i in range(nv):
            prov[i, x] = total([inv[i, j, x] * values[j] for j in range(nv)])
        return carry

    def local_work():
        load_axial.wait()
        load_inverse.wait()
        lax.fori_loop(0, planes, effective, 0)
        load_cross.wait()
        load_source.wait()
        lax.fori_loop(0, planes, flux, 0)

    early = jnp.logical_or(jnp.logical_not(at_start), both(rotor, middle))
    opens_at = jnp.where(early, 0, 3)
    meets_at = jnp.where(at_start, 3, 1)
    load_low.wait()
    load_high.wait()

    def prepare(step, carry):
        pl.when(step == opens_at)(open_up)

        @pl.when(step == 1)
        def _():
            clear()
            load_state.wait()

        pl.when(step == meets_at)(meet_sectors)
        pl.when(step == 2)(local_work)
        return carry

    lax.fori_loop(0, 4, prepare, 0)
    move_picks = pltpu.make_async_copy(picks_wide, picks, local_sem.at[6])
    load_owner.wait()

    @pl.when(on_plane)
    def _():
        shape = (columns, owner.shape[1])
        ids = sector * columns + lax.broadcasted_iota(jnp.int32, shape, 0)
        everyone = lax.broadcasted_iota(jnp.int32, shape, 1)
        owners = jnp.broadcast_to(owner[...], shape)
        is_rotor = jnp.broadcast_to(row, shape) == 0
        hits = jnp.where(is_rotor, everyone, owners) == ids
        found = jnp.sum(
            jnp.where(hits, jnp.where(is_rotor, owners, everyone), 0), axis=1, keepdims=True
        )
        found = jnp.minimum(found, owner.shape[1] - 1)
        picks_wide[...] = jnp.broadcast_to(found, picks_wide.shape)
        move_picks.start()

    place = lax.broadcasted_iota(jnp.int32, (GROUP, cells), 0)

    def mend(side):
        halo_arrival(side).wait_recv()
        at = columns_of(side * (groups - 1))
        touched = place == side * (GROUP - 1)
        scale = jnp.where(side == 0, 0.5, -0.5)

        def one(x, carry):
            outside = [
                jnp.broadcast_to(halo[side, v, x], (GROUP, cells)) for v in range(nv)
            ]
            change = [
                jnp.where(
                    touched,
                    scale * total([cross[0, i, 0, v] * outside[v] for v in range(nv)]),
                    0.0,
                )
                for i in range(nv)
            ]
            for i in range(nv):
                res_out[0, i, x, at] = res_out[0, i, x, at] + change[i]
            for i in range(nv):
                prov[i, x, at] = prov[i, x, at] + total(
                    [inv[i, j, x, at] * change[j] for j in range(nv)]
                )
            return carry

        lax.fori_loop(0, planes, one, 0)

    def gather_facing(*targets):
        move_picks.wait()
        for step in range(1, sectors):
            facing_arrival(step).wait_recv()

        def pick(block, carry):
            for inner in range(GROUP):
                c = block * GROUP + inner
                at = picks[c, 0]
                part, column = at // columns, lax.rem(at, columns)
                for v in range(nv):
                    value = facing[part, v, pl.ds(column, 1)]
                    for target in targets:
                        target[v, pl.ds(c, 1)] = value
            return carry

        lax.fori_loop(0, groups, pick, 0)

    def forward_copy(g):
        return remote(
            leaving.at[:, columns_of(g)], entering.at[:, columns_of(g)],
            fw_send.at[g], fw_recv.at[g], slab=slab + 1,
        )

    def backward_copy(g):
        return remote(
            upd.at[:, columns_of(g)], following.at[:, columns_of(g)],
            bw_send.at[g], bw_recv.at[g], slab=slab - 1,
        )

    def skip_copy(g):
        return remote(
            upd.at[:, columns_of(g)], following.at[:, columns_of(g)],
            skip_send.at[g], bw_recv.at[g], slab=0,
        )

    def base_copy(g):
        return remote(
            upd.at[:, columns_of(g)], base.at[:, columns_of(g)],
            bw_send.at[g], base_recv.at[g], slab=0,
        )

    def mat_copy(g):
        return remote(
            mats_out.at[:, :, columns_of(g)], mats_in.at[:, :, columns_of(g)],
            mat_send.at[g], mat_recv.at[g], slab=slab - 1,
        )

    def blocks_at(x, at):
        return [[eff[i, j, x, at] for j in range(nv)] for i in range(nv)]

    def times(left, right):
        return [
            [total([left[i][j] * right[j][k] for j in range(nv)]) for k in range(nv)]
            for i in range(nv)
        ]

    def pack(matrix):
        return tuple(matrix[i][k] for i in range(nv) for k in range(nv))

    def unpack(values):
        return [list(values[i * nv : i * nv + nv]) for i in range(nv)]

    def store_matrix(g, values):
        at = columns_of(g)
        matrix = unpack(values)
        for i in range(nv):
            for k in range(nv):
                mats_out[i, k, at] = matrix[i][k]

        @pl.when(jnp.logical_or(rotor_top, both(stator, is_second)))
        def _():
            mat_copy(g).start()

    def entry_to_update(step, carry):
        g = lax.rem(step + 1, groups)
        at = columns_of(g)
        first = blocks_at(0, at)
        for i in range(nv):
            for k in range(nv):
                powers[i, k, 0] = first[i][k]

        def up(x, values):
            product = times(blocks_at(x, at), unpack(values))
            for i in range(nv):
                for k in range(nv):
                    powers[i, k, x] = product[i][k]
            return pack(product)

        def down(step, values):
            x = planes - 2 - step
            product = times(blocks_at(x, at), unpack(values))
            return pack(
                [[powers[i, k, x] - product[i][k] for k in range(nv)] for i in range(nv)]
            )

        values = lax.fori_loop(1, planes, up, pack(first))
        store_matrix(g, lax.fori_loop(0, planes - 1, down, values))
        return carry

    def exit_to_update(step, carry):
        g = lax.rem(step + 1, groups)
        at = columns_of(g)

        def down(step, values):
            product = times(blocks_at(planes - 2 - step, at), unpack(values))
            return pack([[-value for value in line] for line in product])

        last = [[-value for value in line] for line in blocks_at(planes - 1, at)]
        store_matrix(g, lax.fori_loop(0, planes - 1, down, pack(last)))
        return carry

    @pl.when(is_last)
    def _():
        lax.fori_loop(0, groups, entry_to_update, 0)

    @pl.when(is_second)
    def _():
        lax.fori_loop(0, groups, exit_to_update, 0)

    def climb(g, now, keep):
        at = columns_of(g)
        for x in range(planes):
            if x == planes - 1:
                now = [now[v] - above[v, at] for v in range(nv)]
            now = [
                total([prov[i, x, at]] + [eff[i, j, x, at] * now[j] for j in range(nv)])
                for i in range(nv)
            ]
            for i in range(nv):
                keep(i, x, now[i])
        return now

    def sweep_up(g):
        at = columns_of(g)

        def keep(i, x, value):
            prov[i, x, at] = value

        now = climb(g, [entering[v, at] for v in range(nv)], keep)

        @pl.when(has_high)
        def _():
            for i in range(nv):
                leaving[i, at] = now[i] + q[i, planes - 1, padded(g)]
            forward_copy(g).start()

    def sweep_down(g, now, known, keep=None):
        at = columns_of(g)
        for x in reversed(range(planes)):
            now = [
                known(i, x) - total([eff[i, j, x, at] * now[j] for j in range(nv)])
                for i in range(nv)
            ]
            if keep is not None:
                keep(x, now)
        return now

    nothing = jnp.zeros((GROUP, cells), jnp.float32)

    def try_alone(g):
        def keep(i, x, value):
            trial[i, x] = value

        climb(g, [nothing] * nv, keep)
        now = sweep_down(g, [nothing] * nv, lambda i, x: trial[i, x])
        for i in range(nv):
            upd[i, columns_of(g)] = now[i]
        backward_copy(g).start()

    def applied(g, added, factor):
        at = columns_of(g)
        return [
            total([added[i, at]] + [mats_in[i, j, at] * factor[j, at] for j in range(nv)])
            for i in range(nv)
        ]

    @pl.when(on_plane)
    def _():
        facing_copy(0).wait_recv()
        for step in range(1, sectors):
            facing_relay(step).start()

    @pl.when(is_last)
    def _():
        @pl.when(rotor)
        def _():
            for g in range(groups):
                mat_copy(g).wait_send()
            pl.semaphore_signal(turn_free, inc=1, device_id=dict(row=1), device_id_type=MESH)

        @pl.when(stator)
        def _():
            pl.semaphore_wait(turn_free, 1)
            for step in range(groups):
                mat_copy((step + 1) % groups).start()

    leads = both(rotor, slab <= 1)
    inside = groups - 2

    def advance(step, carry):
        mends = jnp.where(
            leads, jnp.logical_or(step == inside, step == groups), step < 2
        )
        side = jnp.where(step == jnp.where(leads, inside, 0), 1, 0)
        sweep_at = jnp.where(
            leads, step - (step > inside).astype(jnp.int32) - (step > groups).astype(jnp.int32),
            step - 2,
        )

        @pl.when(mends)
        def _():
            mend(side)

        @pl.when(jnp.logical_not(mends))
        def _():
            g = lax.rem(sweep_at + 1, groups)

            @pl.when(sweep_at == 0)
            def _():
                pl.when(rotor_top)(functools.partial(gather_facing, above))
                pl.when(stator_foot)(functools.partial(gather_facing, entering, below))

            pl.when(is_last)(functools.partial(try_alone, g))

            @pl.when(has_high)
            def _():
                low_copy(g).wait_recv()

            @pl.when(both(has_high, sweep_at == 0))
            def _():
                to_high.start()

            @pl.when(both(has_low, has_high))
            def _():
                forward_copy(g).wait_recv()

            pl.when(has_high)(functools.partial(sweep_up, g))

        return carry

    lax.fori_loop(0, groups + 2, advance, 0)

    @pl.when(is_second)
    def _():
        def ahead(step, carry):
            g = lax.rem(step + 1, groups)
            at = columns_of(g)
            now = sweep_down(g, [nothing] * nv, lambda i, x: prov[i, x, at])
            for i in range(nv):
                upd[i, at] = now[i]
            base_copy(g).start()

            @pl.when(rotor)
            def _():
                mat_copy(g).start()

            return carry

        lax.fori_loop(0, groups, ahead, 0)

    @pl.when(has_low)
    def _():
        to_high.wait_recv()

    for i in range(nv):
        res_out[0, i, 0] = res_out[0, i, 0] + total(
            [(0.5 * axial[i, 0, j]) * below[j] for j in range(nv)]
        )
    for i in range(nv):
        res_out[0, i, planes - 1] = res_out[0, i, planes - 1] - total(
            [(0.5 * axial[i, 0, j]) * above[j] for j in range(nv)]
        )

    to_after.wait_send()
    to_before.wait_send()

    @pl.when(has_high)
    def _():
        to_high.wait_send()

    @pl.when(has_low)
    def _():
        for g in range(groups):
            low_copy(g).wait_send()

    @pl.when(on_plane)
    def _():
        facing_copy(0).wait_send()
        for step in range(1, sectors):
            facing_relay(step).wait_send()

    def back(step, carry):
        g = lax.rem(step + 1, groups)
        at = columns_of(g)

        @pl.when(is_last)
        def _():
            forward_copy(g).wait_recv()
            sweep_up(g)

        @pl.when(has_high)
        def _():
            backward_copy(g).wait_recv()

        @pl.when(is_turn)
        def _():
            mat_copy(g).wait_recv()
            now = applied(g, following, leaving)
            for i in range(nv):
                following[i, at] = now[i]

        @pl.when(is_first)
        def _():
            mat_copy(g).wait_recv()
            base_copy(g).wait_recv()
            now = applied(g, base, following)
            for i in range(nv):
                following[i, at] = now[i]

        def keep(x, now):
            if x == 0:
                @pl.when(both(slab >= 2, has_high))
                def _():
                    for i in range(nv):
                        upd[i, at] = now[i]
                    backward_copy(g).start()

                    @pl.when(is_third)
                    def _():
                        skip_copy(g).start()

            for i in range(nv):
                state_out[0, i, x, at] = q[i, x, padded(g)] + now[i]

        sweep_down(
            g, [following[v, at] for v in range(nv)], lambda i, x: prov[i, x, at], keep
        )
        return carry

    lax.fori_loop(0, groups, back, 0)

    def finish(g, carry):
        @pl.when(has_high)
        def _():
            forward_copy(g).wait_send()

        @pl.when(has_low)
        def _():
            backward_copy(g).wait_send()

        @pl.when(is_third)
        def _():
            skip_copy(g).wait_send()

        @pl.when(jnp.logical_or(both(stator, is_last), is_second))
        def _():
            mat_copy(g).wait_send()

        return carry

    lax.fori_loop(0, groups, finish, 0)


def write_out(res_in, state_in, res_out, state_out, sems):
    first = pltpu.make_async_copy(res_in, res_out, sems.at[0])
    second = pltpu.make_async_copy(state_in, state_out, sems.at[1])
    first.start()
    second.start()
    first.wait()
    second.wait()


def per_device(state, source, diag_inverse, jac_axial, jac_cross, owner):
    _, nv, planes, columns, cells = state.shape
    sectors = lax.axis_size("sector")
    slabs = lax.axis_size("slab")
    groups = columns // GROUP

    def vmem(*shape):
        return pltpu.VMEM(shape, jnp.float32)

    dma = pltpu.SemaphoreType.DMA
    field = (nv, planes, columns, cells)
    plane = (nv, columns, cells)
    outside = pl.BlockSpec(memory_space=pltpu.HBM)
    inside = pl.BlockSpec(memory_space=pltpu.VMEM)
    residual, new_state = pl.pallas_call(
        functools.partial(kernel, sectors, slabs),
        out_shape=[vmem(*state.shape)] * 2,
        in_specs=[outside] * 6,
        out_specs=[inside] * 2,
        scratch_shapes=[
            pltpu.SMEM((nv, 1, nv), jnp.float32),
            pltpu.SMEM((1, nv, 2, nv), jnp.float32),
            pltpu.VMEM((1, owner.shape[0]), jnp.int32),
            pltpu.VMEM((columns, 128), jnp.int32),
            pltpu.SMEM((columns, 128), jnp.int32),
            vmem(nv, planes, columns + 2 * PAD, cells),
            vmem(2, nv, planes, 1, cells),
            vmem(*field),
            vmem(nv, *field),
            vmem(nv, *field),
            vmem(*field),
            vmem(*plane),
            vmem(*plane),
            vmem(sectors, *plane),
            vmem(*plane),
            vmem(*plane),
            vmem(*plane),
            vmem(*plane),
            vmem(*plane),
            vmem(nv, *plane),
            vmem(nv, *plane),
            vmem(nv, nv, planes, GROUP, cells),
            vmem(nv, planes, GROUP, cells),
            dma((9,)),
            dma((1,)), dma((1,)), dma((2,)), dma((2,)),
            dma((sectors,)), dma((sectors,)),
            dma((groups,)), dma((groups,)), dma((groups,)), dma((groups,)),
            dma((groups,)), dma((groups,)), dma((groups,)), dma((groups,)),
            dma((groups,)), dma((groups,)),
            pltpu.SemaphoreType.REGULAR,
            pltpu.SemaphoreType.REGULAR,
        ],
        compiler_params=pltpu.CompilerParams(collective_id=0, has_side_effects=True),
    )(state, source, diag_inverse, jnp.swapaxes(jac_axial, 0, 1),
        jnp.swapaxes(jac_cross, 1, 2), owner[None])
    return pl.pallas_call(
        write_out,
        out_shape=[jax.ShapeDtypeStruct(state.shape, jnp.float32)] * 2,
        in_specs=[inside] * 2,
        out_specs=[outside] * 2,
        scratch_shapes=[dma((2,))],
        compiler_params=pltpu.CompilerParams(vmem_limit_bytes=1 << 20),
    )(
        pltpu.with_memory_space_constraint(residual, pltpu.VMEM),
        pltpu.with_memory_space_constraint(new_state, pltpu.VMEM),
    )


def solution(mesh):
    return jax.shard_map(
        per_device,
        mesh=mesh,
        in_specs=(
            P("row", None, "slab", "sector", None),
            P("row", None, "slab", "sector", None),
            P("row", None, None, "slab", "sector", None),
            P("row", None, None),
            P("row", None, None, None),
            P(),
        ),
        out_specs=(P("row", None, "slab", "sector", None), P("row", None, "slab", "sector", None)),
        check_vma=False,
    )
```

```python
import functools

import jax
import jax.numpy as jnp
from jax import lax
from jax.experimental import pallas as pl
from jax.experimental.pallas import tpu as pltpu
from jax.sharding import PartitionSpec as P

MESH = pl.DeviceIdType.MESH
PAD = 8
GROUP = 8


def total(terms):
    while len(terms) > 1:
        pairs = [a + b for a, b in zip(terms[::2], terms[1::2])]
        if len(terms) % 2:
            pairs.append(terms[-1])
        terms = pairs
    return terms[0]


def both(*conditions):
    return functools.reduce(jnp.logical_and, conditions)


def kernel(
    sectors, slabs,
    state, source, inverse, axial_in, cross_in, owner_in,
    res_out, state_out,
    axial, cross, owner, picks_wide, picks,
    q, halo, src, inv, eff, prov, below, above, facing, entering, following, leaving, upd,
    base, mats_out, mats_in, powers, trial,
    local_sem, ax_send, ax_recv, se_send, se_recv,
    if_send, if_recv, fw_send, fw_recv, bw_send, bw_recv,
    skip_send, base_recv, mat_send, mat_recv, low_send, low_recv, inverse_sem, sectors_in,
):
    nv, planes, columns, cells = src.shape
    groups = columns // GROUP
    row = lax.axis_index("row")
    sector = lax.axis_index("sector")
    slab = lax.axis_index("slab")
    rotor, stator = row == 0, row == 1
    has_low = slab > 0
    has_high = slab < slabs - 1
    is_first, is_last = slab == 0, slab == slabs - 1
    is_second, is_third = slab == 1, slab == 2
    is_turn = slab == slabs - 2
    middle = both(has_low, has_high)
    outer = jnp.logical_or(is_first, is_last)
    rotor_top = both(rotor, is_last)
    stator_foot = both(stator, is_first)
    on_plane = jnp.logical_or(rotor_top, stator_foot)
    after = lax.rem(sector + 1, sectors)
    before = lax.rem(sector + sectors - 1, sectors)
    facing_slab = jnp.where(row == 0, 0, slabs - 1)
    body = pl.ds(PAD, columns)

    def state_copy(first, count, at):
        part = pl.ds(first, count)
        return pltpu.make_async_copy(state.at[0, :, part], q.at[:, part, body], local_sem.at[at])

    load_low, load_high = state_copy(0, 1, 0), state_copy(planes - 1, 1, 7)
    load_state = state_copy(1, planes - 2, 8)
    load_low.start()
    load_high.start()
    load_axial = pltpu.make_async_copy(axial_in, axial, local_sem.at[4])
    load_axial.start()

    def inverse_copy(x):
        return pltpu.make_async_copy(inverse.at[0, :, :, x], inv.at[:, :, x], inverse_sem.at[x])

    for x in range(planes):
        inverse_copy(x).start()
    load_state.start()
    load_cross = pltpu.make_async_copy(cross_in, cross, local_sem.at[5])
    load_cross.start()
    load_owner = pltpu.make_async_copy(owner_in, owner, local_sem.at[3])
    load_owner.start()
    load_source = pltpu.make_async_copy(source.at[0], src, local_sem.at[1])
    load_source.start()

    barrier = pltpu.get_barrier_semaphore()

    def greet(**where):
        pl.semaphore_signal(barrier, inc=1, device_id=where, device_id_type=MESH)

    @pl.when(on_plane)
    def _():
        greet(row=1 - row, slab=facing_slab)
        for step in range(1, sectors):
            greet(sector=lax.rem(sector + step, sectors))

    @pl.when(has_high)
    def _():
        greet(slab=slab + 1)

    beside = both(jnp.logical_or(stator, outer), jnp.logical_not(on_plane))

    @pl.when(beside)
    def _():
        greet(sector=after)
        greet(sector=before)

    @pl.when(both(rotor, middle))
    def _():
        greet(row=1, sector=after)
        greet(row=1, sector=before)
        greet(row=1)

    peers = (
        has_low.astype(jnp.int32)
        + jnp.where(beside, 2, 0)
        + jnp.where(both(stator, middle), 3, 0)
        + jnp.where(on_plane, sectors, 0)
    )

    def remote(source_ref, target_ref, send, recv, **where):
        return pltpu.make_async_remote_copy(
            src_ref=source_ref, dst_ref=target_ref, send_sem=send, recv_sem=recv,
            device_id=where, device_id_type=MESH,
        )

    def columns_of(g):
        return pl.ds(pl.multiple_of(g * GROUP, GROUP), GROUP)

    def padded(g):
        return pl.ds(pl.multiple_of(PAD + g * GROUP, GROUP), GROUP)

    def facing_copy(plane_at, g):
        return remote(
            q.at[:, plane_at, padded(g)], facing.at[sector, :, columns_of(g)],
            if_send.at[0, g], if_recv.at[sector, g], row=1 - row, slab=facing_slab,
        )

    def facing_relay(step, g):
        part = facing.at[sector, :, columns_of(g)]
        return remote(
            part, part, if_send.at[step, g], if_recv.at[sector, g],
            sector=lax.rem(sector + step, sectors),
        )

    def facing_arrival(step, g):
        origin = lax.rem(sector + step, sectors)
        part = facing.at[origin, :, columns_of(g)]
        return remote(part, part, if_send.at[step, g], if_recv.at[origin, g], sector=origin)

    def per_piece(action):
        def one(step, carry):
            for g in range(groups):
                action(step, g)
            return carry

        lax.fori_loop(1, sectors, one, 0)

    to_after = remote(
        q.at[:, :, pl.ds(PAD + columns - 1, 1)], halo.at[0],
        se_send.at[0], se_recv.at[0], sector=after,
    )
    to_before = remote(
        q.at[:, :, pl.ds(PAD, 1)], halo.at[1],
        se_send.at[1], se_recv.at[1], sector=before,
    )

    def halo_arrival(side):
        return remote(
            q.at[:, :, pl.ds(PAD, 1)], halo.at[side],
            se_send.at[side], se_recv.at[side], sector=before,
        )
    to_high = remote(
        q.at[:, planes - 1, body], below, ax_send.at[0], ax_recv.at[0], slab=slab + 1
    )

    def low_copy(g):
        return remote(
            q.at[:, 0, padded(g)], above.at[:, columns_of(g)],
            low_send.at[g], low_recv.at[g], slab=slab - 1,
        )

    def clear():
        zero_plane = jnp.zeros((nv, columns, cells), jnp.float32)
        zero_columns = jnp.zeros((nv, planes, PAD, cells), jnp.float32)
        q[:, :, pl.ds(0, PAD)] = zero_columns
        q[:, :, pl.ds(PAD + columns, PAD)] = zero_columns

        @pl.when(is_first)
        def _():
            entering[...] = zero_plane
            below[...] = zero_plane

        @pl.when(is_last)
        def _():
            following[...] = zero_plane
            above[...] = zero_plane

    at_start = sector == 0

    def open_up():
        pl.semaphore_wait(barrier, peers)

        @pl.when(has_low)
        def _():
            for step in range(groups):
                low_copy((step + 1) % groups).start()

        @pl.when(rotor_top)
        def _():
            for g in range(groups):
                facing_copy(planes - 1, g).start()

        @pl.when(stator_foot)
        def _():
            for g in range(groups):
                facing_copy(0, g).start()

        @pl.when(both(stator, middle))
        def _():
            pl.semaphore_signal(
                sectors_in, inc=1, device_id=dict(row=0), device_id_type=MESH
            )

    def meet_sectors():
        @pl.when(both(rotor, middle))
        def _():
            pl.semaphore_wait(sectors_in, 1)

        to_after.start()
        to_before.start()

    lane = lax.broadcasted_iota(jnp.int32, (columns, cells), 1)
    no_cells = jnp.zeros((columns, cells), jnp.float32)

    def effective(x, carry):
        inverse_copy(x).wait()
        for i in range(nv):
            blocks = [inv[i, j, x] for j in range(nv)]
            for k in range(nv):
                eff[i, k, x] = total([blocks[j] * (0.5 * axial[j, 0, k]) for j in range(nv)])
        return carry

    def flux(x, carry):
        higher = jnp.minimum(x + 1, planes - 1)
        lower = jnp.maximum(x - 1, 0)
        sums = [None] * nv
        for v in range(nv):
            here = q[v, x, body]
            spans = (
                jnp.where(x == planes - 1, no_cells, q[v, higher, body])
                - jnp.where(x == 0, no_cells, q[v, lower, body]),
                q[v, x, pl.ds(PAD + 1, columns)] - q[v, x, pl.ds(PAD - 1, columns)],
                jnp.where(lane == cells - 1, 0.0, pltpu.roll(here, cells - 1, 1))
                - jnp.where(lane == 0, 0.0, pltpu.roll(here, 1, 1)),
            )
            for i in range(nv):
                factors = (axial[i, 0, v], cross[0, i, 0, v], cross[0, i, 1, v])
                term = total([f * s for f, s in zip(factors, spans)])
                sums[i] = term if sums[i] is None else sums[i] + term
        values = [src[i, x] - 0.5 * sums[i] for i in range(nv)]
        for i in range(nv):
            res_out[0, i, x] = values[i]
        for i in range(nv):
            prov[i, x] = total([inv[i, j, x] * values[j] for j in range(nv)])
        return carry

    def mat_copy(g):
        return remote(
            mats_out.at[:, :, columns_of(g)], mats_in.at[:, :, columns_of(g)],
            mat_send.at[g], mat_recv.at[g], slab=slab - 1,
        )

    def blocks_at(x, at):
        return [[eff[i, j, x, at] for j in range(nv)] for i in range(nv)]

    def times(left, right):
        return [
            [total([left[i][j] * right[j][k] for j in range(nv)]) for k in range(nv)]
            for i in range(nv)
        ]

    def pack(matrix):
        return tuple(matrix[i][k] for i in range(nv) for k in range(nv))

    def unpack(values):
        return [list(values[i * nv : i * nv + nv]) for i in range(nv)]

    def store_matrix(g, values):
        at = columns_of(g)
        matrix = unpack(values)
        for i in range(nv):
            for k in range(nv):
                mats_out[i, k, at] = matrix[i][k]

        @pl.when(jnp.logical_or(rotor_top, both(stator, is_second)))
        def _():
            mat_copy(g).start()

    def entry_to_update(step, carry):
        g = lax.rem(step + 1, groups)
        at = columns_of(g)
        first = blocks_at(0, at)
        for i in range(nv):
            for k in range(nv):
                powers[i, k, 0] = first[i][k]

        def up(x, values):
            product = times(blocks_at(x, at), unpack(values))
            for i in range(nv):
                for k in range(nv):
                    powers[i, k, x] = product[i][k]
            return pack(product)

        def down(step, values):
            x = planes - 2 - step
            product = times(blocks_at(x, at), unpack(values))
            return pack(
                [[powers[i, k, x] - product[i][k] for k in range(nv)] for i in range(nv)]
            )

        values = lax.fori_loop(1, planes, up, pack(first))
        store_matrix(g, lax.fori_loop(0, planes - 1, down, values))
        return carry

    def exit_to_update(step, carry):
        g = lax.rem(step + 1, groups)
        at = columns_of(g)

        def down(step, values):
            product = times(blocks_at(planes - 2 - step, at), unpack(values))
            return pack([[-value for value in line] for line in product])

        last = [[-value for value in line] for line in blocks_at(planes - 1, at)]
        store_matrix(g, lax.fori_loop(0, planes - 1, down, pack(last)))
        return carry

    def pass_on():
        def one(g, carry):
            facing_copy(0, g).wait_recv()

            def start(step, carry):
                facing_relay(step, g).start()
                return carry

            return lax.fori_loop(1, sectors, start, carry)

        lax.fori_loop(0, groups, one, 0)

    def matrices():
        @pl.when(is_last)
        def _():
            lax.fori_loop(0, groups, entry_to_update, 0)

        @pl.when(is_second)
        def _():
            lax.fori_loop(0, groups, exit_to_update, 0)

    def products():
        load_axial.wait()
        lax.fori_loop(0, planes, effective, 0)

    def fluxes():
        load_cross.wait()
        load_source.wait()
        lax.fori_loop(0, planes, flux, 0)

    early = jnp.logical_or(jnp.logical_not(at_start), both(rotor, middle))
    opens_at = jnp.where(early, 0, jnp.where(has_low, 3, 6))
    meets_at = jnp.where(at_start, 6, 1)
    passes_at = jnp.where(opens_at > 5, 7, 5)
    load_low.wait()
    load_high.wait()

    def prepare(step, carry):
        pl.when(step == opens_at)(open_up)

        @pl.when(step == 1)
        def _():
            clear()
            load_state.wait()

        pl.when(step == meets_at)(meet_sectors)
        pl.when(step == 2)(products)
        pl.when(step == 4)(matrices)
        pl.when(both(step == passes_at, on_plane))(pass_on)
        pl.when(step == 5)(fluxes)
        return carry

    lax.fori_loop(0, 8, prepare, 0)
    move_picks = pltpu.make_async_copy(picks_wide, picks, local_sem.at[6])
    load_owner.wait()

    @pl.when(on_plane)
    def _():
        shape = (columns, owner.shape[1])
        ids = sector * columns + lax.broadcasted_iota(jnp.int32, shape, 0)
        everyone = lax.broadcasted_iota(jnp.int32, shape, 1)
        owners = jnp.broadcast_to(owner[...], shape)
        is_rotor = jnp.broadcast_to(row, shape) == 0
        hits = jnp.where(is_rotor, everyone, owners) == ids
        found = jnp.sum(
            jnp.where(hits, jnp.where(is_rotor, owners, everyone), 0), axis=1, keepdims=True
        )
        found = jnp.minimum(found, owner.shape[1] - 1)
        picks_wide[...] = jnp.broadcast_to(found, picks_wide.shape)
        move_picks.start()

    place = lax.broadcasted_iota(jnp.int32, (GROUP, cells), 0)

    def mend(side):
        halo_arrival(side).wait_recv()
        at = columns_of(side * (groups - 1))
        touched = place == side * (GROUP - 1)
        scale = jnp.where(side == 0, 0.5, -0.5)

        def one(x, carry):
            outside = [
                jnp.broadcast_to(halo[side, v, x], (GROUP, cells)) for v in range(nv)
            ]
            change = [
                jnp.where(
                    touched,
                    scale * total([cross[0, i, 0, v] * outside[v] for v in range(nv)]),
                    0.0,
                )
                for i in range(nv)
            ]
            for i in range(nv):
                res_out[0, i, x, at] = res_out[0, i, x, at] + change[i]
            for i in range(nv):
                prov[i, x, at] = prov[i, x, at] + total(
                    [inv[i, j, x, at] * change[j] for j in range(nv)]
                )
            return carry

        lax.fori_loop(0, planes, one, 0)

    def gather_facing(*targets):
        move_picks.wait()
        per_piece(lambda step, g: facing_arrival(step, g).wait_recv())

        def pick(block, carry):
            for inner in range(GROUP):
                c = block * GROUP + inner
                at = picks[c, 0]
                part, column = at // columns, lax.rem(at, columns)
                for v in range(nv):
                    value = facing[part, v, pl.ds(column, 1)]
                    for target in targets:
                        target[v, pl.ds(c, 1)] = value
            return carry

        lax.fori_loop(0, groups, pick, 0)

    def forward_copy(g):
        return remote(
            leaving.at[:, columns_of(g)], entering.at[:, columns_of(g)],
            fw_send.at[g], fw_recv.at[g], slab=slab + 1,
        )

    def backward_copy(g):
        return remote(
            upd.at[:, columns_of(g)], following.at[:, columns_of(g)],
            bw_send.at[g], bw_recv.at[g], slab=slab - 1,
        )

    def skip_copy(g):
        return remote(
            upd.at[:, columns_of(g)], following.at[:, columns_of(g)],
            skip_send.at[g], bw_recv.at[g], slab=0,
        )

    def base_copy(g):
        return remote(
            upd.at[:, columns_of(g)], base.at[:, columns_of(g)],
            bw_send.at[g], base_recv.at[g], slab=0,
        )

    def climb(g, now, keep):
        at = columns_of(g)
        for x in range(planes):
            if x == planes - 1:
                now = [now[v] - above[v, at] for v in range(nv)]
            now = [
                total([prov[i, x, at]] + [eff[i, j, x, at] * now[j] for j in range(nv)])
                for i in range(nv)
            ]
            for i in range(nv):
                keep(i, x, now[i])
        return now

    def sweep_up(g):
        at = columns_of(g)

        def keep(i, x, value):
            prov[i, x, at] = value

        now = climb(g, [entering[v, at] for v in range(nv)], keep)

        @pl.when(has_high)
        def _():
            for i in range(nv):
                leaving[i, at] = now[i] + q[i, planes - 1, padded(g)]
            forward_copy(g).start()

    def sweep_down(g, now, known, keep=None):
        at = columns_of(g)
        for x in reversed(range(planes)):
            now = [
                known(i, x) - total([eff[i, j, x, at] * now[j] for j in range(nv)])
                for i in range(nv)
            ]
            if keep is not None:
                keep(x, now)
        return now

    nothing = jnp.zeros((GROUP, cells), jnp.float32)

    def climb_alone(g):
        at = columns_of(g)

        def keep(i, x, value):
            trial[i, x, at] = value

        climb(g, [nothing] * nv, keep)

    def descend_alone(step, carry):
        g = lax.rem(step + 1, groups)
        at = columns_of(g)
        now = sweep_down(
            g, [following[v, at] for v in range(nv)], lambda i, x: trial[i, x, at]
        )
        for i in range(nv):
            upd[i, at] = now[i]
        backward_copy(g).start()
        return carry

    def applied(g, added, factor):
        at = columns_of(g)
        return [
            total([added[i, at]] + [mats_in[i, j, at] * factor[j, at] for j in range(nv)])
            for i in range(nv)
        ]

    at_once = both(stator, is_turn)
    def finish_group(g):
        at = columns_of(g)

        @pl.when(is_last)
        def _():
            forward_copy(g).wait_recv()
            sweep_up(g)

        @pl.when(has_high)
        def _():
            backward_copy(g).wait_recv()

        @pl.when(is_turn)
        def _():
            mat_copy(g).wait_recv()
            now = applied(g, following, leaving)
            for i in range(nv):
                following[i, at] = now[i]

        @pl.when(is_first)
        def _():
            mat_copy(g).wait_recv()
            base_copy(g).wait_recv()
            now = applied(g, base, following)
            for i in range(nv):
                following[i, at] = now[i]

        def keep(x, now):
            if x == 0:
                @pl.when(both(slab >= 2, has_high))
                def _():
                    for i in range(nv):
                        upd[i, at] = now[i]
                    backward_copy(g).start()

                    @pl.when(is_third)
                    def _():
                        skip_copy(g).start()

            for i in range(nv):
                state_out[0, i, x, at] = q[i, x, padded(g)] + now[i]

        sweep_down(
            g, [following[v, at] for v in range(nv)], lambda i, x: prov[i, x, at], keep
        )

    leads = both(rotor, slab <= 1)
    inside = groups - 2

    def advance(step, carry):
        mends = jnp.where(
            leads, jnp.logical_or(step == inside, step == groups), step < 2
        )
        side = jnp.where(step == jnp.where(leads, inside, 0), 1, 0)
        sweep_at = jnp.where(
            leads, step - (step > inside).astype(jnp.int32) - (step > groups).astype(jnp.int32),
            step - 2,
        )

        @pl.when(mends)
        def _():
            mend(side)

        @pl.when(jnp.logical_not(mends))
        def _():
            g = lax.rem(sweep_at + 1, groups)

            @pl.when(sweep_at == 0)
            def _():
                pl.when(stator_foot)(functools.partial(gather_facing, entering, below))

            pl.when(is_last)(functools.partial(climb_alone, g))

            @pl.when(has_high)
            def _():
                low_copy(g).wait_recv()

            @pl.when(both(has_high, sweep_at == 0))
            def _():
                to_high.start()

            @pl.when(both(has_low, has_high))
            def _():
                forward_copy(g).wait_recv()

            pl.when(has_high)(functools.partial(sweep_up, g))
            pl.when(at_once)(functools.partial(finish_group, g))

        return carry

    lax.fori_loop(0, groups + 2, advance, 0)

    @pl.when(is_last)
    def _():
        pl.when(rotor)(functools.partial(gather_facing, following))
        lax.fori_loop(0, groups, descend_alone, 0)

        @pl.when(stator)
        def _():
            for step in range(groups):
                mat_copy((step + 1) % groups).start()

    @pl.when(is_second)
    def _():
        def ahead(step, carry):
            g = lax.rem(step + 1, groups)
            at = columns_of(g)
            now = sweep_down(g, [nothing] * nv, lambda i, x: prov[i, x, at])
            for i in range(nv):
                upd[i, at] = now[i]
            base_copy(g).start()

            @pl.when(rotor)
            def _():
                mat_copy(g).start()

            return carry

        lax.fori_loop(0, groups, ahead, 0)

    @pl.when(has_low)
    def _():
        to_high.wait_recv()

    for i in range(nv):
        res_out[0, i, 0] = res_out[0, i, 0] + total(
            [(0.5 * axial[i, 0, j]) * below[j] for j in range(nv)]
        )
    def mend_top(beyond):
        for i in range(nv):
            res_out[0, i, planes - 1] = res_out[0, i, planes - 1] - total(
                [(0.5 * axial[i, 0, j]) * beyond[j] for j in range(nv)]
            )

    pl.when(is_last)(functools.partial(mend_top, following))
    pl.when(has_high)(functools.partial(mend_top, above))

    to_after.wait_send()
    to_before.wait_send()

    @pl.when(has_high)
    def _():
        to_high.wait_send()

    @pl.when(has_low)
    def _():
        for g in range(groups):
            low_copy(g).wait_send()

    @pl.when(on_plane)
    def _():
        for g in range(groups):
            facing_copy(0, g).wait_send()
        per_piece(lambda step, g: facing_relay(step, g).wait_send())

    def back(step, carry):
        @pl.when(jnp.logical_not(at_once))
        def _():
            finish_group(lax.rem(step + 1, groups))

        return carry

    lax.fori_loop(0, groups, back, 0)

    def finish(g, carry):
        @pl.when(has_high)
        def _():
            forward_copy(g).wait_send()

        @pl.when(has_low)
        def _():
            backward_copy(g).wait_send()

        @pl.when(is_third)
        def _():
            skip_copy(g).wait_send()

        @pl.when(jnp.logical_or(is_last, is_second))
        def _():
            mat_copy(g).wait_send()

        return carry

    lax.fori_loop(0, groups, finish, 0)


def write_out(res_in, state_in, res_out, state_out, sems):
    first = pltpu.make_async_copy(res_in, res_out, sems.at[0])
    second = pltpu.make_async_copy(state_in, state_out, sems.at[1])
    first.start()
    second.start()
    first.wait()
    second.wait()


def per_device(state, source, diag_inverse, jac_axial, jac_cross, owner):
    _, nv, planes, columns, cells = state.shape
    sectors = lax.axis_size("sector")
    slabs = lax.axis_size("slab")
    groups = columns // GROUP

    def vmem(*shape):
        return pltpu.VMEM(shape, jnp.float32)

    dma = pltpu.SemaphoreType.DMA
    field = (nv, planes, columns, cells)
    plane = (nv, columns, cells)
    outside = pl.BlockSpec(memory_space=pltpu.HBM)
    inside = pl.BlockSpec(memory_space=pltpu.VMEM)
    residual, new_state = pl.pallas_call(
        functools.partial(kernel, sectors, slabs),
        out_shape=[vmem(*state.shape)] * 2,
        in_specs=[outside] * 6,
        out_specs=[inside] * 2,
        scratch_shapes=[
            pltpu.SMEM((nv, 1, nv), jnp.float32),
            pltpu.SMEM((1, nv, 2, nv), jnp.float32),
            pltpu.VMEM((1, owner.shape[0]), jnp.int32),
            pltpu.VMEM((columns, 128), jnp.int32),
            pltpu.SMEM((columns, 128), jnp.int32),
            vmem(nv, planes, columns + 2 * PAD, cells),
            vmem(2, nv, planes, 1, cells),
            vmem(*field),
            vmem(nv, *field),
            vmem(nv, *field),
            vmem(*field),
            vmem(*plane),
            vmem(*plane),
            vmem(sectors, *plane),
            vmem(*plane),
            vmem(*plane),
            vmem(*plane),
            vmem(*plane),
            vmem(*plane),
            vmem(nv, *plane),
            vmem(nv, *plane),
            vmem(nv, nv, planes, GROUP, cells),
            vmem(*field),
            dma((9,)),
            dma((1,)), dma((1,)), dma((2,)), dma((2,)),
            dma((sectors, groups)), dma((sectors, groups)),
            dma((groups,)), dma((groups,)), dma((groups,)), dma((groups,)),
            dma((groups,)), dma((groups,)), dma((groups,)), dma((groups,)),
            dma((groups,)), dma((groups,)), dma((planes,)),
            pltpu.SemaphoreType.REGULAR,
        ],
        compiler_params=pltpu.CompilerParams(collective_id=0, has_side_effects=True),
    )(state, source, diag_inverse, jnp.swapaxes(jac_axial, 0, 1),
        jnp.swapaxes(jac_cross, 1, 2), owner[None])
    return pl.pallas_call(
        write_out,
        out_shape=[jax.ShapeDtypeStruct(state.shape, jnp.float32)] * 2,
        in_specs=[inside] * 2,
        out_specs=[outside] * 2,
        scratch_shapes=[dma((2,))],
        compiler_params=pltpu.CompilerParams(vmem_limit_bytes=1 << 20),
    )(
        pltpu.with_memory_space_constraint(residual, pltpu.VMEM),
        pltpu.with_memory_space_constraint(new_state, pltpu.VMEM),
    )


def solution(mesh):
    return jax.shard_map(
        per_device,
        mesh=mesh,
        in_specs=(
            P("row", None, "slab", "sector", None),
            P("row", None, "slab", "sector", None),
            P("row", None, None, "slab", "sector", None),
            P("row", None, None),
            P("row", None, None, None),
            P(),
        ),
        out_specs=(P("row", None, "slab", "sector", None), P("row", None, "slab", "sector", None)),
        check_vma=False,
    )
```

```python
import functools

import jax
import jax.numpy as jnp
from jax import lax
from jax.experimental import pallas as pl
from jax.experimental.pallas import tpu as pltpu
from jax.sharding import PartitionSpec as P

MESH = pl.DeviceIdType.MESH
PAD = 8
GROUP = 8


def total(terms):
    while len(terms) > 1:
        pairs = [a + b for a, b in zip(terms[::2], terms[1::2])]
        if len(terms) % 2:
            pairs.append(terms[-1])
        terms = pairs
    return terms[0]


def both(*conditions):
    return functools.reduce(jnp.logical_and, conditions)


def kernel(
    sectors, slabs,
    state, source, inverse, axial_in, cross_in, owner_in,
    res_out, state_out,
    axial, cross, owner, picks_wide, picks,
    q, halo, src, inv, eff, prov, below, above, facing, entering, following, leaving, upd,
    base, mats_out, mats_in, powers, trial,
    local_sem, ax_send, ax_recv, se_send, se_recv,
    if_send, if_recv, fw_send, fw_recv, bw_send, bw_recv,
    skip_send, base_recv, mat_send, mat_recv, low_send, low_recv, inverse_sem, sectors_in,
):
    nv, planes, columns, cells = src.shape
    groups = columns // GROUP
    row = lax.axis_index("row")
    sector = lax.axis_index("sector")
    slab = lax.axis_index("slab")
    rotor, stator = row == 0, row == 1
    has_low = slab > 0
    has_high = slab < slabs - 1
    is_first, is_last = slab == 0, slab == slabs - 1
    is_second, is_third = slab == 1, slab == 2
    is_turn = slab == slabs - 2
    middle = both(has_low, has_high)
    outer = jnp.logical_or(is_first, is_last)
    rotor_top = both(rotor, is_last)
    stator_foot = both(stator, is_first)
    on_plane = jnp.logical_or(rotor_top, stator_foot)
    after = lax.rem(sector + 1, sectors)
    before = lax.rem(sector + sectors - 1, sectors)
    facing_slab = jnp.where(row == 0, 0, slabs - 1)
    body = pl.ds(PAD, columns)

    def state_copy(first, count, at):
        part = pl.ds(first, count)
        return pltpu.make_async_copy(state.at[0, :, part], q.at[:, part, body], local_sem.at[at])

    load_low, load_high = state_copy(0, 1, 0), state_copy(planes - 1, 1, 7)
    load_state = state_copy(1, planes - 2, 8)
    load_low.start()
    load_high.start()
    load_axial = pltpu.make_async_copy(axial_in, axial, local_sem.at[4])
    load_axial.start()

    def inverse_copy(x):
        return pltpu.make_async_copy(inverse.at[0, :, :, x], inv.at[:, :, x], inverse_sem.at[x])

    for x in range(planes):
        inverse_copy(x).start()
    load_state.start()
    load_cross = pltpu.make_async_copy(cross_in, cross, local_sem.at[5])
    load_cross.start()
    load_owner = pltpu.make_async_copy(owner_in, owner, local_sem.at[3])
    load_owner.start()
    load_source = pltpu.make_async_copy(source.at[0], src, local_sem.at[1])
    load_source.start()

    barrier = pltpu.get_barrier_semaphore()

    def greet(**where):
        pl.semaphore_signal(barrier, inc=1, device_id=where, device_id_type=MESH)

    @pl.when(on_plane)
    def _():
        greet(row=1 - row, slab=facing_slab)
        for step in range(1, sectors):
            greet(sector=lax.rem(sector + step, sectors))

    @pl.when(has_high)
    def _():
        greet(slab=slab + 1)

    beside = both(jnp.logical_or(stator, outer), jnp.logical_not(on_plane))

    @pl.when(beside)
    def _():
        greet(sector=after)
        greet(sector=before)

    @pl.when(both(rotor, middle))
    def _():
        greet(row=1, sector=after)
        greet(row=1, sector=before)
        greet(row=1)

    peers = (
        has_low.astype(jnp.int32)
        + jnp.where(beside, 2, 0)
        + jnp.where(both(stator, middle), 3, 0)
        + jnp.where(on_plane, sectors, 0)
    )

    def remote(source_ref, target_ref, send, recv, **where):
        return pltpu.make_async_remote_copy(
            src_ref=source_ref, dst_ref=target_ref, send_sem=send, recv_sem=recv,
            device_id=where, device_id_type=MESH,
        )

    def columns_of(g):
        return pl.ds(pl.multiple_of(g * GROUP, GROUP), GROUP)

    def padded(g):
        return pl.ds(pl.multiple_of(PAD + g * GROUP, GROUP), GROUP)

    def facing_copy(plane_at, g):
        return remote(
            q.at[:, plane_at, padded(g)], facing.at[sector, :, columns_of(g)],
            if_send.at[0, g], if_recv.at[sector, g], row=1 - row, slab=facing_slab,
        )

    def facing_relay(step, g):
        part = facing.at[sector, :, columns_of(g)]
        return remote(
            part, part, if_send.at[step, g], if_recv.at[sector, g],
            sector=lax.rem(sector + step, sectors),
        )

    def facing_arrival(step, g):
        origin = lax.rem(sector + step, sectors)
        part = facing.at[origin, :, columns_of(g)]
        return remote(part, part, if_send.at[step, g], if_recv.at[origin, g], sector=origin)

    def per_piece(action):
        def one(step, carry):
            for g in range(groups):
                action(step, g)
            return carry

        lax.fori_loop(1, sectors, one, 0)

    to_after = remote(
        q.at[:, :, pl.ds(PAD + columns - 1, 1)], halo.at[0],
        se_send.at[0], se_recv.at[0], sector=after,
    )
    to_before = remote(
        q.at[:, :, pl.ds(PAD, 1)], halo.at[1],
        se_send.at[1], se_recv.at[1], sector=before,
    )

    def halo_arrival(side):
        return remote(
            q.at[:, :, pl.ds(PAD, 1)], halo.at[side],
            se_send.at[side], se_recv.at[side], sector=before,
        )
    to_high = remote(
        q.at[:, planes - 1, body], below, ax_send.at[0], ax_recv.at[0], slab=slab + 1
    )

    def low_copy(g):
        return remote(
            q.at[:, 0, padded(g)], above.at[:, columns_of(g)],
            low_send.at[g], low_recv.at[g], slab=slab - 1,
        )

    def clear():
        zero_plane = jnp.zeros((nv, columns, cells), jnp.float32)
        zero_columns = jnp.zeros((nv, planes, PAD, cells), jnp.float32)
        q[:, :, pl.ds(0, PAD)] = zero_columns
        q[:, :, pl.ds(PAD + columns, PAD)] = zero_columns

        @pl.when(is_first)
        def _():
            entering[...] = zero_plane
            below[...] = zero_plane

        @pl.when(is_last)
        def _():
            following[...] = zero_plane
            above[...] = zero_plane

    at_start = sector == 0

    def open_up():
        pl.semaphore_wait(barrier, peers)

        @pl.when(has_low)
        def _():
            for step in range(groups):
                low_copy((step + 1) % groups).start()

        @pl.when(rotor_top)
        def _():
            for g in range(groups):
                facing_copy(planes - 1, g).start()

        @pl.when(stator_foot)
        def _():
            for g in range(groups):
                facing_copy(0, g).start()

        @pl.when(both(stator, middle))
        def _():
            pl.semaphore_signal(
                sectors_in, inc=1, device_id=dict(row=0), device_id_type=MESH
            )

    def meet_sectors():
        @pl.when(both(rotor, middle))
        def _():
            pl.semaphore_wait(sectors_in, 1)

        to_after.start()
        to_before.start()

    lane = lax.broadcasted_iota(jnp.int32, (columns, cells), 1)
    no_cells = jnp.zeros((columns, cells), jnp.float32)

    def effective(x, carry):
        inverse_copy(x).wait()
        for i in range(nv):
            blocks = [inv[i, j, x] for j in range(nv)]
            for k in range(nv):
                eff[i, k, x] = total([blocks[j] * (0.5 * axial[j, 0, k]) for j in range(nv)])
        return carry

    def flux(x, carry):
        higher = jnp.minimum(x + 1, planes - 1)
        lower = jnp.maximum(x - 1, 0)
        sums = [None] * nv
        for v in range(nv):
            here = q[v, x, body]
            spans = (
                jnp.where(x == planes - 1, no_cells, q[v, higher, body])
                - jnp.where(x == 0, no_cells, q[v, lower, body]),
                q[v, x, pl.ds(PAD + 1, columns)] - q[v, x, pl.ds(PAD - 1, columns)],
                jnp.where(lane == cells - 1, 0.0, pltpu.roll(here, cells - 1, 1))
                - jnp.where(lane == 0, 0.0, pltpu.roll(here, 1, 1)),
            )
            for i in range(nv):
                factors = (axial[i, 0, v], cross[0, i, 0, v], cross[0, i, 1, v])
                term = total([f * s for f, s in zip(factors, spans)])
                sums[i] = term if sums[i] is None else sums[i] + term
        values = [src[i, x] - 0.5 * sums[i] for i in range(nv)]
        for i in range(nv):
            res_out[0, i, x] = values[i]
        for i in range(nv):
            prov[i, x] = total([inv[i, j, x] * values[j] for j in range(nv)])
        return carry

    def mat_copy(g):
        return remote(
            mats_out.at[:, :, columns_of(g)], mats_in.at[:, :, columns_of(g)],
            mat_send.at[g], mat_recv.at[g], slab=slab - 1,
        )

    def blocks_at(x, at):
        return [[eff[i, j, x, at] for j in range(nv)] for i in range(nv)]

    def times(left, right):
        return [
            [total([left[i][j] * right[j][k] for j in range(nv)]) for k in range(nv)]
            for i in range(nv)
        ]

    def pack(matrix):
        return tuple(matrix[i][k] for i in range(nv) for k in range(nv))

    def unpack(values):
        return [list(values[i * nv : i * nv + nv]) for i in range(nv)]

    def store_matrix(g, values):
        at = columns_of(g)
        matrix = unpack(values)
        for i in range(nv):
            for k in range(nv):
                mats_out[i, k, at] = matrix[i][k]

        @pl.when(jnp.logical_or(rotor_top, both(stator, is_second)))
        def _():
            mat_copy(g).start()

    def entry_to_update(step, carry):
        g = lax.rem(step + 1, groups)
        at = columns_of(g)
        first = blocks_at(0, at)
        for i in range(nv):
            for k in range(nv):
                powers[i, k, 0] = first[i][k]

        def up(x, values):
            product = times(blocks_at(x, at), unpack(values))
            for i in range(nv):
                for k in range(nv):
                    powers[i, k, x] = product[i][k]
            return pack(product)

        def down(step, values):
            x = planes - 2 - step
            product = times(blocks_at(x, at), unpack(values))
            return pack(
                [[powers[i, k, x] - product[i][k] for k in range(nv)] for i in range(nv)]
            )

        values = lax.fori_loop(1, planes, up, pack(first))
        store_matrix(g, lax.fori_loop(0, planes - 1, down, values))
        return carry

    def exit_to_update(step, carry):
        g = lax.rem(step + 1, groups)
        at = columns_of(g)

        def down(step, values):
            product = times(blocks_at(planes - 2 - step, at), unpack(values))
            return pack([[-value for value in line] for line in product])

        last = [[-value for value in line] for line in blocks_at(planes - 1, at)]
        store_matrix(g, lax.fori_loop(0, planes - 1, down, pack(last)))
        return carry

    def pass_on():
        def one(g, carry):
            facing_copy(0, g).wait_recv()

            def start(step, carry):
                facing_relay(step, g).start()
                return carry

            return lax.fori_loop(1, sectors, start, carry)

        lax.fori_loop(0, groups, one, 0)

    def matrices():
        @pl.when(is_last)
        def _():
            lax.fori_loop(0, groups, entry_to_update, 0)

        @pl.when(is_second)
        def _():
            lax.fori_loop(0, groups, exit_to_update, 0)

    def products():
        load_axial.wait()
        lax.fori_loop(0, planes, effective, 0)

    def fluxes():
        load_cross.wait()
        load_source.wait()
        lax.fori_loop(0, planes, flux, 0)

    early = jnp.logical_or(jnp.logical_not(at_start), both(rotor, middle))
    opens_at = jnp.where(early, 0, 3)
    meets_at = jnp.where(at_start, 6, 1)
    passes_at = jnp.where(opens_at > 5, 7, 5)
    load_low.wait()
    load_high.wait()

    def prepare(step, carry):
        pl.when(step == opens_at)(open_up)

        @pl.when(step == 1)
        def _():
            clear()
            load_state.wait()

        pl.when(step == meets_at)(meet_sectors)
        pl.when(step == 2)(products)
        pl.when(step == 4)(matrices)
        pl.when(both(step == passes_at, on_plane))(pass_on)
        pl.when(step == 5)(fluxes)
        return carry

    lax.fori_loop(0, 8, prepare, 0)
    move_picks = pltpu.make_async_copy(picks_wide, picks, local_sem.at[6])
    load_owner.wait()

    @pl.when(on_plane)
    def _():
        shape = (columns, owner.shape[1])
        ids = sector * columns + lax.broadcasted_iota(jnp.int32, shape, 0)
        everyone = lax.broadcasted_iota(jnp.int32, shape, 1)
        owners = jnp.broadcast_to(owner[...], shape)
        is_rotor = jnp.broadcast_to(row, shape) == 0
        hits = jnp.where(is_rotor, everyone, owners) == ids
        found = jnp.sum(
            jnp.where(hits, jnp.where(is_rotor, owners, everyone), 0), axis=1, keepdims=True
        )
        found = jnp.minimum(found, owner.shape[1] - 1)
        picks_wide[...] = jnp.broadcast_to(found, picks_wide.shape)
        move_picks.start()

    place = lax.broadcasted_iota(jnp.int32, (GROUP, cells), 0)

    def mend(side):
        halo_arrival(side).wait_recv()
        at = columns_of(side * (groups - 1))
        touched = place == side * (GROUP - 1)
        scale = jnp.where(side == 0, 0.5, -0.5)

        def one(x, carry):
            outside = [
                jnp.broadcast_to(halo[side, v, x], (GROUP, cells)) for v in range(nv)
            ]
            change = [
                jnp.where(
                    touched,
                    scale * total([cross[0, i, 0, v] * outside[v] for v in range(nv)]),
                    0.0,
                )
                for i in range(nv)
            ]
            for i in range(nv):
                res_out[0, i, x, at] = res_out[0, i, x, at] + change[i]
            for i in range(nv):
                prov[i, x, at] = prov[i, x, at] + total(
                    [inv[i, j, x, at] * change[j] for j in range(nv)]
                )
            return carry

        lax.fori_loop(0, planes, one, 0)

    def gather_facing(*targets):
        move_picks.wait()
        per_piece(lambda step, g: facing_arrival(step, g).wait_recv())

        def pick(block, carry):
            for inner in range(GROUP):
                c = block * GROUP + inner
                at = picks[c, 0]
                part, column = at // columns, lax.rem(at, columns)
                for v in range(nv):
                    value = facing[part, v, pl.ds(column, 1)]
                    for target in targets:
                        target[v, pl.ds(c, 1)] = value
            return carry

        lax.fori_loop(0, groups, pick, 0)

    def forward_copy(g):
        return remote(
            leaving.at[:, columns_of(g)], entering.at[:, columns_of(g)],
            fw_send.at[g], fw_recv.at[g], slab=slab + 1,
        )

    def backward_copy(g):
        return remote(
            upd.at[:, columns_of(g)], following.at[:, columns_of(g)],
            bw_send.at[g], bw_recv.at[g], slab=slab - 1,
        )

    def skip_copy(g):
        return remote(
            upd.at[:, columns_of(g)], following.at[:, columns_of(g)],
            skip_send.at[g], bw_recv.at[g], slab=0,
        )

    def base_copy(g):
        return remote(
            upd.at[:, columns_of(g)], base.at[:, columns_of(g)],
            bw_send.at[g], base_recv.at[g], slab=0,
        )

    def climb(g, now, keep):
        at = columns_of(g)
        for x in range(planes):
            if x == planes - 1:
                now = [now[v] - above[v, at] for v in range(nv)]
            now = [
                total([prov[i, x, at]] + [eff[i, j, x, at] * now[j] for j in range(nv)])
                for i in range(nv)
            ]
            for i in range(nv):
                keep(i, x, now[i])
        return now

    def sweep_up(g):
        at = columns_of(g)

        def keep(i, x, value):
            prov[i, x, at] = value

        now = climb(g, [entering[v, at] for v in range(nv)], keep)

        @pl.when(has_high)
        def _():
            for i in range(nv):
                leaving[i, at] = now[i] + q[i, planes - 1, padded(g)]
            forward_copy(g).start()

    def sweep_down(g, now, known, keep=None):
        at = columns_of(g)
        for x in reversed(range(planes)):
            now = [
                known(i, x) - total([eff[i, j, x, at] * now[j] for j in range(nv)])
                for i in range(nv)
            ]
            if keep is not None:
                keep(x, now)
        return now

    nothing = jnp.zeros((GROUP, cells), jnp.float32)

    def climb_alone(g):
        at = columns_of(g)

        def keep(i, x, value):
            trial[i, x, at] = value

        climb(g, [nothing] * nv, keep)

    def descend_alone(step, carry):
        g = lax.rem(step + 1, groups)
        at = columns_of(g)
        now = sweep_down(
            g, [following[v, at] for v in range(nv)], lambda i, x: trial[i, x, at]
        )
        for i in range(nv):
            upd[i, at] = now[i]
        backward_copy(g).start()
        return carry

    def applied(g, added, factor):
        at = columns_of(g)
        return [
            total([added[i, at]] + [mats_in[i, j, at] * factor[j, at] for j in range(nv)])
            for i in range(nv)
        ]

    at_once = both(stator, is_turn)
    def finish_group(g):
        at = columns_of(g)

        @pl.when(is_last)
        def _():
            forward_copy(g).wait_recv()
            sweep_up(g)

        @pl.when(has_high)
        def _():
            backward_copy(g).wait_recv()

        @pl.when(is_turn)
        def _():
            mat_copy(g).wait_recv()
            now = applied(g, following, leaving)
            for i in range(nv):
                following[i, at] = now[i]

        @pl.when(is_first)
        def _():
            mat_copy(g).wait_recv()
            base_copy(g).wait_recv()
            now = applied(g, base, following)
            for i in range(nv):
                following[i, at] = now[i]

        def keep(x, now):
            if x == 0:
                @pl.when(both(slab >= 2, has_high))
                def _():
                    for i in range(nv):
                        upd[i, at] = now[i]
                    backward_copy(g).start()

                    @pl.when(is_third)
                    def _():
                        skip_copy(g).start()

            for i in range(nv):
                state_out[0, i, x, at] = q[i, x, padded(g)] + now[i]

        sweep_down(
            g, [following[v, at] for v in range(nv)], lambda i, x: prov[i, x, at], keep
        )

    leads = both(rotor, slab <= 1)
    inside = groups - 2

    def advance(step, carry):
        mends = jnp.where(
            leads, jnp.logical_or(step == inside, step == groups), step < 2
        )
        side = jnp.where(step == jnp.where(leads, inside, 0), 1, 0)
        sweep_at = jnp.where(
            leads, step - (step > inside).astype(jnp.int32) - (step > groups).astype(jnp.int32),
            step - 2,
        )

        @pl.when(mends)
        def _():
            mend(side)

        @pl.when(jnp.logical_not(mends))
        def _():
            g = lax.rem(sweep_at + 1, groups)

            @pl.when(sweep_at == 0)
            def _():
                pl.when(stator_foot)(functools.partial(gather_facing, entering, below))

            pl.when(is_last)(functools.partial(climb_alone, g))

            @pl.when(has_high)
            def _():
                low_copy(g).wait_recv()

            @pl.when(both(has_high, sweep_at == 0))
            def _():
                to_high.start()

            @pl.when(both(has_low, has_high))
            def _():
                forward_copy(g).wait_recv()

            pl.when(has_high)(functools.partial(sweep_up, g))
            pl.when(at_once)(functools.partial(finish_group, g))

        return carry

    lax.fori_loop(0, groups + 2, advance, 0)

    @pl.when(is_last)
    def _():
        pl.when(rotor)(functools.partial(gather_facing, following))
        lax.fori_loop(0, groups, descend_alone, 0)

        @pl.when(stator)
        def _():
            for step in range(groups):
                mat_copy((step + 1) % groups).start()

    @pl.when(is_second)
    def _():
        def ahead(step, carry):
            g = lax.rem(step + 1, groups)
            at = columns_of(g)
            now = sweep_down(g, [nothing] * nv, lambda i, x: prov[i, x, at])
            for i in range(nv):
                upd[i, at] = now[i]
            base_copy(g).start()

            @pl.when(rotor)
            def _():
                mat_copy(g).start()

            return carry

        lax.fori_loop(0, groups, ahead, 0)

    @pl.when(has_low)
    def _():
        to_high.wait_recv()

    for i in range(nv):
        res_out[0, i, 0] = res_out[0, i, 0] + total(
            [(0.5 * axial[i, 0, j]) * below[j] for j in range(nv)]
        )
    def mend_top(beyond):
        for i in range(nv):
            res_out[0, i, planes - 1] = res_out[0, i, planes - 1] - total(
                [(0.5 * axial[i, 0, j]) * beyond[j] for j in range(nv)]
            )

    pl.when(is_last)(functools.partial(mend_top, following))
    pl.when(has_high)(functools.partial(mend_top, above))

    to_after.wait_send()
    to_before.wait_send()

    @pl.when(has_high)
    def _():
        to_high.wait_send()

    @pl.when(has_low)
    def _():
        for g in range(groups):
            low_copy(g).wait_send()

    @pl.when(on_plane)
    def _():
        for g in range(groups):
            facing_copy(0, g).wait_send()
        per_piece(lambda step, g: facing_relay(step, g).wait_send())

    def back(step, carry):
        @pl.when(jnp.logical_not(at_once))
        def _():
            finish_group(lax.rem(step + 1, groups))

        return carry

    lax.fori_loop(0, groups, back, 0)

    def finish(g, carry):
        @pl.when(has_high)
        def _():
            forward_copy(g).wait_send()

        @pl.when(has_low)
        def _():
            backward_copy(g).wait_send()

        @pl.when(is_third)
        def _():
            skip_copy(g).wait_send()

        @pl.when(jnp.logical_or(is_last, is_second))
        def _():
            mat_copy(g).wait_send()

        return carry

    lax.fori_loop(0, groups, finish, 0)


def write_out(res_in, state_in, res_out, state_out, sems):
    first = pltpu.make_async_copy(res_in, res_out, sems.at[0])
    second = pltpu.make_async_copy(state_in, state_out, sems.at[1])
    first.start()
    second.start()
    first.wait()
    second.wait()


def per_device(state, source, diag_inverse, jac_axial, jac_cross, owner):
    _, nv, planes, columns, cells = state.shape
    sectors = lax.axis_size("sector")
    slabs = lax.axis_size("slab")
    groups = columns // GROUP

    def vmem(*shape):
        return pltpu.VMEM(shape, jnp.float32)

    dma = pltpu.SemaphoreType.DMA
    field = (nv, planes, columns, cells)
    plane = (nv, columns, cells)
    outside = pl.BlockSpec(memory_space=pltpu.HBM)
    inside = pl.BlockSpec(memory_space=pltpu.VMEM)
    residual, new_state = pl.pallas_call(
        functools.partial(kernel, sectors, slabs),
        out_shape=[vmem(*state.shape)] * 2,
        in_specs=[outside] * 6,
        out_specs=[inside] * 2,
        scratch_shapes=[
            pltpu.SMEM((nv, 1, nv), jnp.float32),
            pltpu.SMEM((1, nv, 2, nv), jnp.float32),
            pltpu.VMEM((1, owner.shape[0]), jnp.int32),
            pltpu.VMEM((columns, 128), jnp.int32),
            pltpu.SMEM((columns, 128), jnp.int32),
            vmem(nv, planes, columns + 2 * PAD, cells),
            vmem(2, nv, planes, 1, cells),
            vmem(*field),
            vmem(nv, *field),
            vmem(nv, *field),
            vmem(*field),
            vmem(*plane),
            vmem(*plane),
            vmem(sectors, *plane),
            vmem(*plane),
            vmem(*plane),
            vmem(*plane),
            vmem(*plane),
            vmem(*plane),
            vmem(nv, *plane),
            vmem(nv, *plane),
            vmem(nv, nv, planes, GROUP, cells),
            vmem(*field),
            dma((9,)),
            dma((1,)), dma((1,)), dma((2,)), dma((2,)),
            dma((sectors, groups)), dma((sectors, groups)),
            dma((groups,)), dma((groups,)), dma((groups,)), dma((groups,)),
            dma((groups,)), dma((groups,)), dma((groups,)), dma((groups,)),
            dma((groups,)), dma((groups,)), dma((planes,)),
            pltpu.SemaphoreType.REGULAR,
        ],
        compiler_params=pltpu.CompilerParams(collective_id=0, has_side_effects=True),
    )(state, source, diag_inverse, jnp.swapaxes(jac_axial, 0, 1),
        jnp.swapaxes(jac_cross, 1, 2), owner[None])
    return pl.pallas_call(
        write_out,
        out_shape=[jax.ShapeDtypeStruct(state.shape, jnp.float32)] * 2,
        in_specs=[inside] * 2,
        out_specs=[outside] * 2,
        scratch_shapes=[dma((2,))],
        compiler_params=pltpu.CompilerParams(vmem_limit_bytes=1 << 20),
    )(
        pltpu.with_memory_space_constraint(residual, pltpu.VMEM),
        pltpu.with_memory_space_constraint(new_state, pltpu.VMEM),
    )


def solution(mesh):
    return jax.shard_map(
        per_device,
        mesh=mesh,
        in_specs=(
            P("row", None, "slab", "sector", None),
            P("row", None, "slab", "sector", None),
            P("row", None, None, "slab", "sector", None),
            P("row", None, None),
            P("row", None, None, None),
            P(),
        ),
        out_specs=(P("row", None, "slab", "sector", None), P("row", None, "slab", "sector", None)),
        check_vma=False,
    )
```
